32 devices in a mesh: tile: 16 (over z, y, core), shell: 2 (over x).
Axes of the slice: x: 2, y: 2, z: 4, core: 2. Of those that a mesh axis runs over, the one named last changes fastest.
Arguments:
- particles: bfloat16 [512, 2, 32768], P('tile', None, 'shell'), may hold values from -40 to 40
- projections: bfloat16 [512, 2, 32768], P('tile', None, 'shell'), may hold values from -6 to 6
- noise_weight: float32 [32768], P('shell'), may hold values from 0.001 to 0.012
- tile_list: int32 [512, 4], P('tile'), may hold values from 0 to 15, all different within a row; in each aligned block of 32 rows (0 to 31, 32 to 63, ...) at most 16 rows name the same one
- ori_start: int32 [512, 4], P('tile'), may hold values from 0 to 31
- shifts: int32 [512, 2], P('tile'), may hold values from -8 to 8
- defocus_bin: int32 [512], P('tile'), may hold values from 0 to 15
Outputs:
- posterior: float32 [512, 9, 64], P('tile')
- log_evidence: float32 [512], P('tile')
The draws below stay inside these ranges and needn't reach their ends.
Inputs may be any that keep to these rules, and one draw needn't show every extreme that they name: `tile_list`: the 4 tiles of one particle differ, and among the particles of one index of tile no tile is named more than 16 times, a count reached.
All inputs are finite; a program needn't handle non-finite values.
Results may differ from the reference program's by a relative error of at most 0.0035.
Values may be sent and summed in bfloat16 or wider, within the bound.
A program may use at most 192 MiB of HBM per device.

```python
import math
import jax
import jax.numpy as jnp
import numpy as np
from jax import lax

BOX = 256
K = 32768
ORI_DEV = 32
ORI_WIN = 16
N_ORI = 512
WIN = 4
P_DEV = 32
PARTICLES = 512
CAP = 16
NBIN = 16
TSIDE = 3
N_TILE = 16


def draw_particles(key, part):
    scale_key = jax.random.fold_in(key, 11)
    noise_key = jax.random.fold_in(key, 12)
    gauss = jax.random.normal(noise_key, (PARTICLES, 2, K), jnp.float32)
    scales = jnp.exp(jax.random.uniform(scale_key, (PARTICLES, 1, 1), jnp.float32, math.log(2.0), math.log(8.0)))
    values = scales * gauss
    return jnp.clip(values, -40.0, 40.0).astype(jnp.bfloat16)


def draw_projections(key, part):
    tile_key = jax.random.fold_in(key, 22)

    def one_tile(tile_index):
        block_key = jax.random.fold_in(tile_key, tile_index)
        raw = jax.random.normal(block_key, (ORI_DEV, 2, K), jnp.float32)
        spread = jnp.sqrt(jnp.mean(raw * raw, axis=(1, 2), keepdims=True))
        return jnp.clip(raw / spread, -6.0, 6.0).astype(jnp.bfloat16)
    tiles = lax.map(one_tile, jnp.arange(N_TILE, dtype=jnp.int32))
    return tiles.reshape(N_ORI, 2, K)


def touch_ends(drawn, rng, least, top_value):
    extent = drawn.shape
    place = [jax.random.randint(jax.random.fold_in(rng, axis), (), 0, extent[axis]) for axis in range(len(extent))]
    drawn = drawn.at[tuple(place)].set(least)
    longest = extent.index(max(extent))
    place[longest] = (place[longest] + 1) % extent[longest]
    return drawn.at[tuple(place)].set(top_value)


def block_levels(own_key, shape, pieces, least, top_value):
    factor_of, own = 1.0, jax.random.fold_in(own_key, 6)
    for axis_at, shards_of in pieces:
        steps = jnp.exp(jax.random.uniform(jax.random.fold_in(own, axis_at), (shards_of,), jnp.float32, least / len(pieces), top_value / len(pieces)))
        factor_of = factor_of * jnp.repeat(steps, shape[axis_at] // shards_of).reshape([-1 if axis == axis_at else 1 for axis in range(len(shape))])
    return factor_of


def routed_block(rng, own, number, rows, amount, top, most, slope):
    ranking = jax.random.permutation(rng, amount)
    crowded, ordinary = shares(amount, rows * top, most, slope, True), shares(amount, rows * top, most, slope, False)
    places = jnp.arange(amount)

    def named(lengths, turn):
        used = int((lengths > 0).sum())
        fixed = max(1, used // 4)
        passed = fixed + (places - fixed + turn * (used - fixed)) % max(1, amount - fixed)
        return jnp.zeros((amount,), jnp.int32).at[ranking[jnp.where(places < fixed, places, passed)]].set(jnp.asarray(lengths, jnp.int32))

    lengths = jnp.where(number % 4 == 0, named(crowded, number // 4), named(ordinary, number - number // 4 - 1))
    mixed = jax.random.permutation(jax.random.fold_in(own, 3), amount)
    giver, receiver = mixed[0:amount // 2 * 2:2], mixed[1:amount // 2 * 2:2]
    slack = jnp.minimum(lengths[giver] - 1, most - lengths[receiver]) // 2
    slack = jnp.where((giver == ranking[0]) | (receiver == ranking[0]) | (lengths[receiver] == 0), 0, jnp.maximum(slack, 0))
    passed = jax.random.randint(jax.random.fold_in(own, 4), (amount // 2,), 0, 1 << 20) % (slack + 1)
    lengths = lengths.at[giver].add(-passed).at[receiver].add(passed)
    items = jnp.searchsorted(jnp.cumsum(lengths), jnp.arange(rows * top), side="right").astype(jnp.int32)
    table = items.reshape(top, rows).T
    table = table[jax.random.permutation(jax.random.fold_in(own, 1), rows)]
    turn = jax.random.randint(jax.random.fold_in(own, 2), (rows, 1), 0, top)
    return jnp.take_along_axis(table, (jnp.arange(top)[None, :] + turn) % top, axis=1)


def shares(amount, total, most, lean, full):
    weights = [(1 << 20) // math.isqrt(grade ** lean) + 1 for grade in range(1, amount + 1)]
    largest = most if full else min(most, max(-(-total // amount), total * weights[0] // sum(weights)))
    least = 1 if total - largest >= amount - 1 else 0
    holding, surplus = [largest] + [least] * (amount - 1), total - largest - least * (amount - 1)
    while surplus > 0:
        free = [i for i in range(1, amount) if holding[i] < largest] or [i for i in range(1, amount) if holding[i] < most]
        pool, left = sum([weights[i] for i in free]), surplus
        for i in free:
            more = min(most - holding[i], max(1, left * weights[i] // pool), surplus)
            holding[i] = holding[i] + more
            surplus = surplus - more
    return np.array(holding)


def setup_inputs(seed: int = 0) -> dict:
    key_of = jax.random.split(jax.random.key(seed), 8)
    particles = draw_particles(jax.random.fold_in(key_of[7], 71), 0)
    projections = draw_projections(jax.random.fold_in(key_of[7], 71), 0)
    noise_weight = jnp.clip(jnp.exp(math.log(0.012) - 2.4849066 * jax.random.uniform(key_of[2], (K,), jnp.float32) ** block_levels(key_of[2], (K,), ((0, 2),), -0.2, 0.2)), 0.001, 0.012)
    tile_list_keys = jax.random.split(jax.random.fold_in(key_of[3], 1), PARTICLES // P_DEV)
    tile_list_turns = jax.random.permutation(jax.random.fold_in(key_of[3], 3), PARTICLES // P_DEV)
    tile_list = jax.vmap(lambda own, number: routed_block(jax.random.fold_in(key_of[3], 2), own, number, P_DEV, N_TILE, WIN, CAP, 2))(tile_list_keys, tile_list_turns).reshape((PARTICLES, WIN))
    ori_start = touch_ends(jax.random.randint(key_of[4], (PARTICLES, WIN), 0, ORI_DEV), jax.random.fold_in(key_of[4], 1), 0, ORI_DEV - 1).astype(jnp.int32)
    shifts = touch_ends(jax.random.randint(key_of[5], (PARTICLES, 2), -8, 9), jax.random.fold_in(key_of[5], 1), -8, 8).astype(jnp.int32)
    defocus_bin = touch_ends(jax.random.randint(key_of[6], (PARTICLES,), 0, NBIN), jax.random.fold_in(key_of[6], 1), 0, NBIN - 1).astype(jnp.int32)
    return {"particles": particles, "projections": projections, "noise_weight": noise_weight, "tile_list": tile_list, "ori_start": ori_start, "shifts": shifts, "defocus_bin": defocus_bin}


wave_length = 0.0197
aberration = 27000000.0
amplitude = 0.1
b_factor = 20.0
defocus_base = 5000.0
defocus_step = 500.0

def frequencies(first_index, span_count):
    flat_index = first_index + jnp.arange(span_count, dtype=jnp.int32)
    freq_x = flat_index // BOX
    freq_y = flat_index % BOX - BOX // 2
    return (freq_x, freq_y)

def ctf_table(freq_x, freq_y, bins_count):
    scaled_x = freq_x.astype(jnp.float32) / BOX
    scaled_y = freq_y.astype(jnp.float32) / BOX
    radius_sq = scaled_x * scaled_x + scaled_y * scaled_y
    defocus = defocus_base + defocus_step * jnp.arange(bins_count, dtype=jnp.float32)[:, None]
    aberr_phase = math.pi * wave_length * defocus * radius_sq[None, :] - 0.5 * math.pi * aberration * wave_length ** 3 * radius_sq[None, :] ** 2
    envelope = jnp.exp(-0.25 * b_factor * radius_sq)[None, :]
    return -(math.sqrt(1.0 - amplitude ** 2) * jnp.sin(aberr_phase) + amplitude * jnp.cos(aberr_phase)) * envelope

def rotation(freq_x, freq_y, mult_x, mult_y):
    phase_turns = jnp.mod(freq_x * mult_x + freq_y * mult_y, BOX)
    angles = phase_turns.astype(jnp.float32) * (2.0 * math.pi / BOX)
    return (jnp.cos(angles), jnp.sin(angles))

def pick_rows(bin_index, lookup):
    one_hot = (bin_index[:, None] == jnp.arange(lookup.shape[0], dtype=jnp.int32)[None, :]).astype(jnp.float32)
    return jnp.dot(one_hot, lookup, precision=lax.Precision.HIGHEST, preferred_element_type=jnp.float32)

def prepare(particles, weight, ctf_rows, shifts, freq_x, freq_y):
    values = particles.astype(jnp.float32)
    real_part = values[:, 0]
    imag_part = values[:, 1]
    cosine, sine_value = rotation(freq_x[None, :], freq_y[None, :], shifts[:, 0:1], shifts[:, 1:2])
    moved_real = real_part * cosine + imag_part * sine_value
    moved_imag = imag_part * cosine - real_part * sine_value
    factor = weight[None, :] * ctf_rows
    weighted = jnp.stack([factor * moved_real, factor * moved_imag], axis=1).astype(jnp.bfloat16)
    energy = lax.optimization_barrier(jnp.sum(weight[None, :] * (real_part * real_part + imag_part * imag_part), axis=1))
    return (weighted, energy)

def shifted_tables(projections, freq_x, freq_y):
    offsets = jnp.arange(TSIDE, dtype=jnp.int32) - TSIDE // 2
    mult_x = jnp.repeat(offsets, TSIDE)[:, None]
    mult_y = jnp.tile(offsets, TSIDE)[:, None]
    cosine, sine_value = rotation(freq_x[None, :], freq_y[None, :], mult_x, mult_y)
    cosine = cosine[:, None, :]
    sine_value = sine_value[:, None, :]
    proj_real = projections[:, 0].astype(jnp.float32)[None, :, :]
    proj_imag = projections[:, 1].astype(jnp.float32)[None, :, :]
    moved_real = proj_real * cosine - proj_imag * sine_value
    moved_imag = proj_imag * cosine + proj_real * sine_value
    stacked = jnp.stack([moved_real, moved_imag], axis=2).astype(jnp.bfloat16)
    return stacked.reshape(TSIDE * TSIDE * projections.shape[0], -1)

def slot_scores(slot_rows, bin_index, projections, weight, ctf, freq_x, freq_y):
    orient_count = projections.shape[0]
    lookup = shifted_tables(projections, freq_x, freq_y)
    cross_term = lax.dot_general(slot_rows, lookup, (((1,), (1,)), ((), ())), preferred_element_type=jnp.float32)
    cross_term = cross_term.reshape(slot_rows.shape[0], TSIDE * TSIDE, orient_count)
    proj_values = projections.astype(jnp.float32)
    magnitude = proj_values[:, 0] * proj_values[:, 0] + proj_values[:, 1] * proj_values[:, 1]
    weighted_ctf = weight[None, :] * ctf * ctf
    power = lax.dot_general(weighted_ctf, magnitude, (((1,), (1,)), ((), ())), precision=lax.Precision.HIGHEST, preferred_element_type=jnp.float32)
    power_rows = pick_rows(bin_index, power)
    return cross_term - 0.5 * power_rows[:, None, :]

def window(scores, starts, orient_count):
    orient_index = jnp.mod(starts[:, None] + jnp.arange(orient_count // 2, dtype=jnp.int32)[None, :], orient_count)
    return jnp.take_along_axis(scores, orient_index[:, None, :], axis=2)

def slot_layout(tile_ids, tile_count, capacity):
    positions = jnp.arange(tile_ids.shape[0], dtype=jnp.int32)
    earlier_same = (tile_ids[:, None] == tile_ids[None, :]) & (positions[None, :] < positions[:, None])
    slot_rank = lax.optimization_barrier(jnp.sum(earlier_same.astype(jnp.int32), axis=1))
    slot_index = tile_ids * capacity + slot_rank
    matches = slot_index[None, :] == jnp.arange(tile_count * capacity, dtype=jnp.int32)[:, None]
    slot_owner = lax.optimization_barrier(jnp.sum(jnp.where(matches, positions[None, :] + 1, 0), axis=1)) - 1
    return (slot_index, slot_owner)

def finish(scores, energy_sum):
    scored = scores - 0.5 * energy_sum[:, None, None]
    row_peak = lax.optimization_barrier(jnp.max(scored, axis=(1, 2)))
    log_total = row_peak + jnp.log(lax.optimization_barrier(jnp.sum(jnp.exp(scored - row_peak[:, None, None]), axis=(1, 2))))
    posterior = jnp.exp(scored - log_total[:, None, None])
    return (posterior, log_total)

def reference(particles, projections, noise_weight, tile_list, ori_start, shifts, defocus_bin):
    capacity = CAP
    freq_x, freq_y = frequencies(0, K)
    ctf = ctf_table(freq_x, freq_y, NBIN)

    def prep_block(block_index):
        first = block_index * P_DEV
        block_particles = lax.dynamic_slice_in_dim(particles, first, P_DEV, 0)
        block_shifts = lax.dynamic_slice_in_dim(shifts, first, P_DEV, 0)
        block_bins = lax.dynamic_slice_in_dim(defocus_bin, first, P_DEV, 0)
        return prepare(block_particles, noise_weight, pick_rows(block_bins, ctf), block_shifts, freq_x, freq_y)
    weighted, energy = lax.map(prep_block, jnp.arange(N_TILE, dtype=jnp.int32))
    weighted = weighted.reshape(PARTICLES, 2 * K)
    energy = energy.reshape(PARTICLES)
    block_tiles = tile_list.reshape(N_TILE, P_DEV * WIN)
    slots_all, owners_all = jax.vmap(lambda tile_ids: slot_layout(tile_ids, N_TILE, capacity))(block_tiles)
    starts_flat = ori_start.reshape(-1)

    def score_tile(tile_index):
        slot_owner = lax.dynamic_slice_in_dim(owners_all, tile_index * capacity, capacity, 1)
        source_index = jnp.arange(N_TILE, dtype=jnp.int32)[:, None]
        item_index = (source_index * (P_DEV * WIN) + jnp.maximum(slot_owner, 0)).reshape(-1)
        particle = item_index // WIN
        occupied = (slot_owner >= 0).reshape(-1)
        slot_rows = jnp.where(occupied[:, None], weighted[particle], jnp.zeros((), weighted.dtype))
        tile_proj = lax.dynamic_slice_in_dim(projections, tile_index * ORI_DEV, ORI_DEV, 0)
        partial_value = slot_scores(slot_rows, defocus_bin[particle], tile_proj, noise_weight, ctf, freq_x, freq_y)
        chosen = window(partial_value, starts_flat[item_index], ORI_DEV)
        return chosen.reshape(N_TILE, capacity, TSIDE * TSIDE, ORI_WIN)
    results = lax.map(score_tile, jnp.arange(N_TILE, dtype=jnp.int32))
    tiles_flat = tile_list.reshape(-1)
    source_of = jnp.arange(PARTICLES * WIN, dtype=jnp.int32) // (P_DEV * WIN)
    slot_rank = slots_all.reshape(-1) - tiles_flat * capacity
    returned = results[tiles_flat, source_of, slot_rank]
    returned = returned.reshape(PARTICLES, WIN, TSIDE * TSIDE, ORI_WIN)
    scores = jnp.transpose(returned, (0, 2, 1, 3)).reshape(PARTICLES, TSIDE * TSIDE, WIN * ORI_WIN)
    return finish(scores, energy)
```

```python
import functools
import math

import jax
import jax.numpy as jnp
from jax import lax
from jax.experimental import pallas as pl
from jax.experimental.pallas import tpu as pltpu
from jax.sharding import PartitionSpec as P

BOX = 256
NBIN = 16
TSIDE = 3


wave_length = 0.0197
aberration = 27000000.0
amplitude = 0.1
b_factor = 20.0
defocus_base = 5000.0
defocus_step = 500.0


def frequencies(first_index, span_count):
    flat_index = first_index + jnp.arange(span_count, dtype=jnp.int32)
    freq_x = flat_index // BOX
    freq_y = flat_index % BOX - BOX // 2
    return (freq_x, freq_y)


def ctf_table(freq_x, freq_y, bins_count):
    scaled_x = freq_x.astype(jnp.float32) / BOX
    scaled_y = freq_y.astype(jnp.float32) / BOX
    radius_sq = scaled_x * scaled_x + scaled_y * scaled_y
    defocus = defocus_base + defocus_step * jnp.arange(bins_count, dtype=jnp.float32)[:, None]
    aberr_phase = (
        math.pi * wave_length * defocus * radius_sq[None, :]
        - 0.5 * math.pi * aberration * wave_length**3 * radius_sq[None, :] ** 2
    )
    envelope = jnp.exp(-0.25 * b_factor * radius_sq)[None, :]
    return (
        -(math.sqrt(1.0 - amplitude**2) * jnp.sin(aberr_phase) + amplitude * jnp.cos(aberr_phase))
        * envelope
    )


def rotation(freq_x, freq_y, mult_x, mult_y):
    phase_turns = jnp.mod(freq_x * mult_x + freq_y * mult_y, BOX)
    angles = phase_turns.astype(jnp.float32) * (2.0 * math.pi / BOX)
    return (jnp.cos(angles), jnp.sin(angles))


def pick_rows(bin_index, lookup):
    one_hot = (bin_index[:, None] == jnp.arange(lookup.shape[0], dtype=jnp.int32)[None, :]).astype(
        jnp.float32
    )
    return jnp.dot(
        one_hot, lookup, precision=lax.Precision.HIGHEST, preferred_element_type=jnp.float32
    )


def prepare(particles, weight, ctf_rows, shifts, freq_x, freq_y):
    values = particles.astype(jnp.float32)
    real_part = values[:, 0]
    imag_part = values[:, 1]
    cosine, sine_value = rotation(freq_x[None, :], freq_y[None, :], shifts[:, 0:1], shifts[:, 1:2])
    moved_real = real_part * cosine + imag_part * sine_value
    moved_imag = imag_part * cosine - real_part * sine_value
    factor = weight[None, :] * ctf_rows
    weighted = jnp.stack([factor * moved_real, factor * moved_imag], axis=1).astype(jnp.bfloat16)
    energy = jnp.sum(weight[None, :] * (real_part * real_part + imag_part * imag_part), axis=1)
    return (weighted, energy)


def shifted_tables(projections, freq_x, freq_y):
    offsets = jnp.arange(TSIDE, dtype=jnp.int32) - TSIDE // 2
    mult_x = jnp.repeat(offsets, TSIDE)[:, None]
    mult_y = jnp.tile(offsets, TSIDE)[:, None]
    cosine, sine_value = rotation(freq_x[None, :], freq_y[None, :], mult_x, mult_y)
    cosine = cosine[:, None, :]
    sine_value = sine_value[:, None, :]
    proj_real = projections[:, 0].astype(jnp.float32)[None, :, :]
    proj_imag = projections[:, 1].astype(jnp.float32)[None, :, :]
    moved_real = proj_real * cosine - proj_imag * sine_value
    moved_imag = proj_imag * cosine + proj_real * sine_value
    stacked = jnp.stack([moved_real, moved_imag], axis=2).astype(jnp.bfloat16)
    return stacked.reshape(TSIDE * TSIDE * projections.shape[0], -1)


def slot_scores(slot_rows, bin_index, projections, weight, ctf, freq_x, freq_y):
    orient_count = projections.shape[0]
    lookup = shifted_tables(projections, freq_x, freq_y)
    cross_term = lax.dot_general(
        slot_rows, lookup, (((1,), (1,)), ((), ())), preferred_element_type=jnp.float32
    )
    cross_term = cross_term.reshape(slot_rows.shape[0], TSIDE * TSIDE, orient_count)
    proj_values = projections.astype(jnp.float32)
    magnitude = proj_values[:, 0] * proj_values[:, 0] + proj_values[:, 1] * proj_values[:, 1]
    weighted_ctf = weight[None, :] * ctf * ctf
    power = lax.dot_general(
        weighted_ctf,
        magnitude,
        (((1,), (1,)), ((), ())),
        precision=lax.Precision.HIGHEST,
        preferred_element_type=jnp.float32,
    )
    power_rows = pick_rows(bin_index, power)
    return cross_term - 0.5 * power_rows[:, None, :]


def window(scores, starts, orient_count):
    orient_index = jnp.mod(
        starts[:, None] + jnp.arange(orient_count // 2, dtype=jnp.int32)[None, :], orient_count
    )
    return jnp.take_along_axis(scores, orient_index[:, None, :], axis=2)


def slot_layout(tile_ids, tile_count, capacity):
    positions = jnp.arange(tile_ids.shape[0], dtype=jnp.int32)
    earlier_same = (tile_ids[:, None] == tile_ids[None, :]) & (
        positions[None, :] < positions[:, None]
    )
    slot_rank = jnp.sum(earlier_same.astype(jnp.int32), axis=1)
    slot_index = tile_ids * capacity + slot_rank
    matches = slot_index[None, :] == jnp.arange(tile_count * capacity, dtype=jnp.int32)[:, None]
    slot_owner = jnp.sum(jnp.where(matches, positions[None, :] + 1, 0), axis=1) - 1
    return (slot_index, slot_owner)


def finish(scores, energy_sum):
    scored = scores - 0.5 * energy_sum[:, None, None]
    row_peak = jnp.max(scored, axis=(1, 2))
    log_total = row_peak + jnp.log(jnp.sum(jnp.exp(scored - row_peak[:, None, None]), axis=(1, 2)))
    posterior = jnp.exp(scored - log_total[:, None, None])
    return (posterior, log_total)


def slot_plan(particles, projections, noise_weight, tile_list, ori_start, shifts, defocus_bin):
    tile_count = lax.axis_size("tile")
    band_index = lax.axis_index("shell")
    local_count = particles.shape[0]
    window_count = tile_list.shape[1]
    band_width = particles.shape[2]
    orient_count = projections.shape[0]
    capacity = max(2, (2 * local_count * window_count + tile_count - 1) // tile_count)
    freq_x, freq_y = frequencies(band_index * band_width, band_width)
    ctf = ctf_table(freq_x, freq_y, NBIN)
    weighted, energy = prepare(
        particles, noise_weight, pick_rows(defocus_bin, ctf), shifts, freq_x, freq_y
    )
    weighted = weighted.reshape(local_count, 2 * band_width)
    slot_index, slot_owner = slot_layout(tile_list.reshape(-1), tile_count, capacity)
    occupied = slot_owner >= 0
    item_index = jnp.maximum(slot_owner, 0)
    particle = item_index // window_count
    starts_flat = ori_start.reshape(-1)
    send_rows = jnp.where(
        occupied[:, None], jnp.take(weighted, particle, axis=0), jnp.zeros((), jnp.bfloat16)
    )
    send_rows = send_rows.reshape(tile_count, capacity, 2 * band_width)
    send_labels = jnp.stack(
        [jnp.take(defocus_bin, particle), jnp.take(starts_flat, item_index)], axis=1
    )
    send_labels = send_labels.astype(jnp.bfloat16).reshape(tile_count, capacity, 2)
    payload = lax.all_to_all(send_rows, "tile", split_axis=0, concat_axis=0, tiled=True)
    labels = lax.all_to_all(send_labels, "tile", split_axis=0, concat_axis=0, tiled=True)
    source_count = payload.shape[0]
    slot_count = payload.shape[1]
    slot_rows = payload.reshape(source_count * slot_count, payload.shape[2])
    label_ints = labels.reshape(source_count * slot_count, 2).astype(jnp.int32)
    partial_value = slot_scores(
        slot_rows, label_ints[:, 0], projections, noise_weight, ctf, freq_x, freq_y
    )
    partial_value = partial_value.reshape(
        source_count, slot_count, partial_value.shape[1], partial_value.shape[2]
    )
    returned = lax.all_to_all(partial_value, "tile", split_axis=0, concat_axis=0, tiled=True)
    candidates = returned.shape[2]
    returned = jnp.take(
        returned.reshape(tile_count * capacity, candidates, returned.shape[3]), slot_index, axis=0
    )
    returned = window(returned, starts_flat, orient_count)
    kept = returned.shape[2]
    returned = returned.reshape(local_count, window_count, candidates, kept)
    scores = jnp.transpose(returned, (0, 2, 1, 3)).reshape(
        local_count, candidates, window_count * kept
    )
    scores, energy_sum = lax.psum((scores, energy), "shell")
    return finish(scores, energy_sum)


SHIFT_MAX = 8
HIGH = lax.Precision.HIGHEST


def round_up(value, step):
    return (value + step - 1) // step * step


LANES = 128
MESH = pl.DeviceIdType.MESH


def flip(index, turn, count):
    result = index
    step = 1
    while step < count:
        result = result + step * (turn // step % 2) * (1 - 2 * (index // step % 2))
        step *= 2
    return result


def offset_of(order, fars):
    far = (fars - order // 4) % fars
    return far * 4 + order % 2 * 2 + order % 4 // 2


def place_of(order, fars):
    return order % 4 * fars + (fars - order // 4) % fars


def fused_kernel(
    windows,
    part_ref,
    proj_ref,
    label_ref,
    turn_y_ref,
    turn_x_ref,
    weight_ref,
    ctf_ref,
    ctf_sq_ref,
    cos_ref,
    sin_ref,
    post_ref,
    log_ref,
    part_in,
    proj_in,
    label_in,
    hot,
    wave_y,
    wave_x,
    factor,
    weighted,
    square_sum,
    plain,
    magnitude,
    moved,
    sums,
    core_in,
    side_in,
    far_out,
    far_in,
    pair_out,
    pair_in,
    own_sems,
    send_sems,
    recv_sems,
    back_send,
    back_recv,
):
    tile_count, rows, lines, _ = part_in.shape
    fars = tile_count // 4
    orients = proj_in.shape[1]
    kept = orients // 2
    cands = TSIDE * TSIDE
    middle = cands // 2
    width = weight_ref.shape[1]
    chunks = width // LANES
    band_rows = width // BOX
    count = weighted.shape[0]
    half_windows = windows // 2
    used = cands * half_windows * kept
    me = lax.axis_index("tile")
    band = lax.axis_index("shell")
    other = 1 - band
    core_peer = flip(me, 1, tile_count)
    side_peer = flip(me, 2, tile_count)

    barrier = pltpu.get_barrier_semaphore()
    peers = [(flip(me, offset, tile_count), band) for offset in range(1, tile_count)]
    peers += [(me, other), (side_peer, other)]
    for peer in peers:
        pl.semaphore_signal(barrier, inc=1, device_id=peer, device_id_type=MESH)
    pl.semaphore_wait(barrier, len(peers))

    def remote(source, target, send, recv, peer):
        return pltpu.make_async_remote_copy(
            src_ref=source,
            dst_ref=target,
            send_sem=send,
            recv_sem=recv,
            device_id=peer,
            device_id_type=MESH,
        )

    def piece(ref, tile):
        return ref.at[:, pl.ds(pl.multiple_of(tile * lines, lines), lines), :]

    sent = []
    own_copies = []
    for kind, (source, target) in enumerate(
        ((label_ref, label_in), (part_ref, part_in), (proj_ref, proj_in))
    ):
        if kind:
            copy = pltpu.make_async_copy(piece(source, me), target.at[0], own_sems.at[kind - 1])
            copy.start()
            own_copies.append(copy)
        for order in range(1, tile_count):
            tile = flip(me, offset_of(order, fars), tile_count)
            block = piece(source, tile) if kind else source.at[place_of(order, fars) % fars]
            copy = remote(
                block,
                target.at[order],
                send_sems.at[kind, order],
                recv_sems.at[kind, order],
                (tile, band),
            )
            copy.start()
            sent.append(copy)

    def arrived(kind, target, order):
        remote(
            target.at[order],
            target.at[order],
            send_sems.at[kind, order],
            recv_sems.at[kind, order],
            (core_peer, band),
        ).wait_recv()

    sums[...] = jnp.zeros_like(sums)
    label_in[0] = label_ref[0]
    for order in range(1, tile_count):
        arrived(0, label_in, order)
    groups = []
    for group in range(4):
        total = None
        for order in range(group, tile_count, 4):
            value = label_in[order].astype(jnp.float32)
            total = value if total is None else total + value
        groups.append(total)
    labels = jnp.concatenate(groups, axis=1)
    tiles = [labels[j : j + 1] for j in range(windows)]
    starts = [labels[windows + j : windows + j + 1] for j in range(windows)]
    shift_x = labels[2 * windows : 2 * windows + 1]
    shift_y = labels[2 * windows + 1 : 2 * windows + 2]
    bins = labels[2 * windows + 2 : 2 * windows + 3]

    def one_hot(row, table_rows, base):
        index = lax.broadcasted_iota(jnp.int32, (table_rows, count), 0).astype(jnp.float32)
        return (index == row + base).astype(jnp.float32)

    def pick(one_hots, table):
        return lax.dot_general(
            one_hots,
            table,
            (((0,), (0,)), ((), ())),
            precision=HIGH,
            preferred_element_type=jnp.float32,
        )

    steps = turn_y_ref.shape[0]
    hot[...] = one_hot(bins, NBIN, 0.0)
    wave_y[...] = pick(one_hot(shift_y, steps, float(SHIFT_MAX)), turn_y_ref[...])
    wave_x[...] = pick(one_hot(shift_x, steps, float(SHIFT_MAX)), turn_x_ref[...])
    factor[...] = pick(hot[...], ctf_ref[...])

    def unpack(value):
        plain[...] = value.reshape(rows * lines, LANES).astype(jnp.float32)

    def parts_of(chunk):
        real_part = plain[pl.ds(2 * chunk, rows, stride=lines), :]
        imag_part = plain[pl.ds(2 * chunk + 1, rows, stride=lines), :]
        return real_part, imag_part

    for copy in own_copies:
        copy.wait()

    def weigh(order, carry):
        @pl.when(order > 0)
        def _():
            arrived(1, part_in, order)

        unpack(part_in[order])
        first = pl.multiple_of(place_of(order, fars) * rows, rows)
        span = pl.ds(first, rows)
        energy = jnp.zeros((rows, LANES), jnp.float32)
        for chunk in range(chunks):
            line, side = divmod(chunk, BOX // LANES)
            real_part, imag_part = parts_of(chunk)
            cos_y = wave_y[span, side * LANES : (side + 1) * LANES]
            sin_y = wave_y[span, BOX + side * LANES : BOX + (side + 1) * LANES]
            cos_x = wave_x[span, line : line + 1]
            sin_x = wave_x[span, band_rows + line : band_rows + line + 1]
            cosine = cos_x * cos_y - sin_x * sin_y
            sine_value = sin_x * cos_y + cos_x * sin_y
            columns = slice(chunk * LANES, (chunk + 1) * LANES)
            scale = factor[span, columns]
            weighted[span, columns] = (
                scale * (real_part * cosine + imag_part * sine_value)
            ).astype(jnp.bfloat16)
            weighted[span, width + chunk * LANES : width + (chunk + 1) * LANES] = (
                scale * (imag_part * cosine - real_part * sine_value)
            ).astype(jnp.bfloat16)
            square = real_part * real_part + imag_part * imag_part
            energy += weight_ref[:, columns] * square
        square_sum[span, :] = energy
        return carry

    lax.fori_loop(0, tile_count, weigh, 0)
    energy = lax.dot_general(
        jnp.ones((8, LANES), jnp.float32),
        square_sum[...],
        (((1,), (1,)), ((), ())),
        precision=HIGH,
        preferred_element_type=jnp.float32,
    )
    for half in range(2):
        sums[half, used : used + 8, :] = energy

    def score(order, carry):
        @pl.when(order > 0)
        def _():
            arrived(2, proj_in, order)

        unpack(proj_in[order])
        for chunk in range(chunks):
            columns = slice(chunk * LANES, (chunk + 1) * LANES)
            real_part, imag_part = parts_of(chunk)
            magnitude[:, columns] = real_part * real_part + imag_part * imag_part

            def put(cand, real_value, imag_value):
                span = slice(cand * orients, (cand + 1) * orients)
                moved[span, columns] = real_value.astype(jnp.bfloat16)
                moved[span, width + chunk * LANES : width + (chunk + 1) * LANES] = (
                    imag_value.astype(jnp.bfloat16)
                )

            put(middle, real_part, imag_part)
            for cand in range(middle):
                cosine = cos_ref[cand : cand + 1, columns]
                sine_value = sin_ref[cand : cand + 1, columns]
                real_cos = real_part * cosine
                imag_sin = imag_part * sine_value
                imag_cos = imag_part * cosine
                real_sin = real_part * sine_value
                put(cand, real_cos - imag_sin, imag_cos + real_sin)
                put(cands - 1 - cand, real_cos + imag_sin, imag_cos - real_sin)
        power = lax.dot_general(
            magnitude[...],
            ctf_sq_ref[...],
            (((1,), (1,)), ((), ())),
            precision=HIGH,
            preferred_element_type=jnp.float32,
        )
        half_power = 0.5 * jnp.dot(
            power, hot[...], precision=HIGH, preferred_element_type=jnp.float32
        )
        cross = lax.dot_general(
            moved[...],
            weighted[...],
            (((1,), (1,)), ((), ())),
            preferred_element_type=jnp.float32,
        )
        tile = flip(me, offset_of(order, fars), tile_count).astype(jnp.float32)
        named = [row == tile for row in tiles]
        start = jnp.zeros_like(starts[0])
        for j in range(windows):
            start = jnp.where(named[j], starts[j], start)
        start = start.astype(jnp.int32)
        for cand in range(cands):
            value = cross[cand * orients : (cand + 1) * orients] - half_power
            bit = orients // 2
            while bit:
                turned = pltpu.roll(value, orients - bit, 0)
                value = jnp.where((start & bit) != 0, turned, value)
                bit //= 2
            value = value[:kept]
            for j in range(windows):
                half, place = divmod(j, half_windows)
                first = (cand * half_windows + place) * kept
                span = slice(first, first + kept)
                sums[half, span, :] = jnp.where(named[j], value, sums[half, span, :])
        return carry

    lax.fori_loop(0, tile_count, score, 0)

    near = count // 2
    quarter = count // 4
    copy = remote(
        sums.at[:, :, pl.ds(near, near)],
        core_in,
        back_send.at[0],
        back_recv.at[0],
        (core_peer, band),
    )
    copy.start()
    sent.append(copy)
    copy.wait_recv()
    sums[:, :, :near] = sums[:, :, :near] + core_in[...]

    copies = []
    for way, (half, lane, peer) in enumerate(
        (
            (other, quarter, (side_peer, other)),
            (other, 0, (me, other)),
            (band, quarter, (side_peer, band)),
        )
    ):
        copy = remote(
            sums.at[half, :, pl.ds(lane, quarter)],
            side_in.at[way],
            back_send.at[1 + way],
            back_recv.at[1 + way],
            peer,
        )
        copy.start()
        copies.append(copy)
    total = sums[band, :, :quarter]
    for way, copy in enumerate(copies):
        copy.wait_recv()
        total = total + side_in[way]
    sent += copies
    spare = far_out.shape[1] - total.shape[0]
    total = jnp.concatenate([total, jnp.zeros((spare, quarter), jnp.float32)], axis=0)
    far_out[...] = total.T

    copies = []
    for far in range(1, fars):
        copy = remote(
            far_out.at[pl.ds(far * rows, rows), :],
            far_in.at[far],
            back_send.at[3 + far],
            back_recv.at[3 + far],
            (flip(me, 4 * far, tile_count), band),
        )
        copy.start()
        copies.append(copy)
    total = far_out[:rows, :]
    for far, copy in enumerate(copies):
        copy.wait_recv()
        total = total + far_in[1 + far]
    sent += copies
    pair_out[...] = total
    copy = remote(
        pair_out, pair_in, back_send.at[3 + fars], back_recv.at[3 + fars], (me, other)
    )
    copy.start()
    sent.append(copy)
    inside = lax.broadcasted_iota(jnp.int32, total.shape, 1) < used
    low = jnp.full_like(total, -jnp.inf)
    energy = total[:, used : used + 1]
    own = jnp.where(inside, total, low)
    own_peak = jnp.max(own, axis=1, keepdims=True)
    copy.wait_recv()
    theirs = jnp.where(inside, pair_in[...], low)
    peak = jnp.maximum(own_peak, jnp.max(theirs, axis=1, keepdims=True))
    mass = jnp.sum(jnp.exp(own - peak), axis=1, keepdims=True)
    mass += jnp.sum(jnp.exp(theirs - peak), axis=1, keepdims=True)
    log_total = peak + jnp.log(mass)
    post_ref[band] = jnp.exp(own - log_total)
    post_ref[other] = jnp.exp(theirs - log_total)
    log_ref[...] = jnp.broadcast_to(log_total - 0.5 * energy, log_ref.shape)
    for copy in sent:
        copy.wait_send()


def fused_plan(particles, projections, noise_weight, tile_list, ori_start, shifts, defocus_bin):
    tile_count = lax.axis_size("tile")
    tile_index = lax.axis_index("tile")
    band_index = lax.axis_index("shell")
    local_count, pair, band_width = particles.shape
    orients = projections.shape[0]
    windows = tile_list.shape[1]
    width = band_width // tile_count
    lines = width // BOX
    count = local_count * tile_count
    cands = TSIDE * TSIDE
    fars = tile_count // 4
    half_rows = cands * (windows // 2) * (orients // 2) + 8
    columns = round_up(half_rows, LANES)
    piece = width // LANES * pair

    labels = jnp.concatenate([tile_list, ori_start, shifts, defocus_bin[:, None]], axis=1).T
    labels = labels.astype(jnp.bfloat16)
    label_rows = round_up(labels.shape[0], 16)
    labels = jnp.pad(labels, ((0, label_rows - labels.shape[0]), (0, 0)))
    labels = jnp.stack(
        [
            jnp.pad(labels, ((0, 0), (far * local_count, (fars - 1 - far) * local_count)))
            for far in range(fars)
        ]
    )

    freq_x, freq_y = frequencies(band_index * band_width + tile_index * width, width)
    weight = lax.dynamic_slice_in_dim(noise_weight, tile_index * width, width, 0)
    ctf = ctf_table(freq_x, freq_y, NBIN)
    span = round_up(2 * SHIFT_MAX + 1, 8)
    steps = jnp.arange(span, dtype=jnp.int32) - SHIFT_MAX
    none = jnp.zeros((), jnp.int32)
    own_y = jnp.arange(BOX, dtype=jnp.int32) - BOX // 2
    own_x = freq_x[::BOX]
    turn_y = jnp.concatenate(rotation(own_y[None, :], own_y[None, :], none, steps[:, None]), axis=1)
    turn_x = jnp.concatenate(rotation(own_x[None, :], own_x[None, :], steps[:, None], none), axis=1)
    turn_x = jnp.pad(turn_x, ((0, 0), (0, LANES - 2 * lines)))
    offsets = jnp.arange(TSIDE, dtype=jnp.int32) - TSIDE // 2
    cos_t, sin_t = rotation(
        freq_x[None, :],
        freq_y[None, :],
        jnp.repeat(offsets, TSIDE)[:, None],
        jnp.tile(offsets, TSIDE)[:, None],
    )

    def view(values):
        rows = values.shape[0]
        blocks = values.reshape(rows, pair, band_width // LANES, LANES)
        return jnp.transpose(blocks, (0, 2, 1, 3)).reshape(rows, -1, LANES)

    far_space = pl.BlockSpec(memory_space=pl.ANY)
    near_space = pl.BlockSpec(memory_space=pltpu.VMEM)
    posterior, log_total = pl.pallas_call(
        functools.partial(fused_kernel, windows),
        in_specs=[far_space] * 2 + [near_space] * 8,
        out_specs=[near_space] * 2,
        out_shape=[
            jax.ShapeDtypeStruct((2, local_count, columns), jnp.float32),
            jax.ShapeDtypeStruct((local_count, LANES), jnp.float32),
        ],
        scratch_shapes=[
            pltpu.VMEM((tile_count, local_count, piece, LANES), jnp.bfloat16),
            pltpu.VMEM((tile_count, orients, piece, LANES), jnp.bfloat16),
            pltpu.VMEM((tile_count, label_rows, LANES), jnp.bfloat16),
            pltpu.VMEM((NBIN, count), jnp.float32),
            pltpu.VMEM((count, 2 * BOX), jnp.float32),
            pltpu.VMEM((count, LANES), jnp.float32),
            pltpu.VMEM((count, width), jnp.float32),
            pltpu.VMEM((count, pair * width), jnp.bfloat16),
            pltpu.VMEM((count, LANES), jnp.float32),
            pltpu.VMEM((local_count * piece, LANES), jnp.float32),
            pltpu.VMEM((orients, width), jnp.float32),
            pltpu.VMEM((cands * orients, pair * width), jnp.bfloat16),
            pltpu.VMEM((2, half_rows, count), jnp.float32),
            pltpu.VMEM((2, half_rows, count // 2), jnp.float32),
            pltpu.VMEM((3, half_rows, count // 4), jnp.float32),
            pltpu.VMEM((count // 4, columns), jnp.float32),
            pltpu.VMEM((fars, local_count, columns), jnp.float32),
            pltpu.VMEM((local_count, columns), jnp.float32),
            pltpu.VMEM((local_count, columns), jnp.float32),
            pltpu.SemaphoreType.DMA((2,)),
            pltpu.SemaphoreType.DMA((3, tile_count)),
            pltpu.SemaphoreType.DMA((3, tile_count)),
            pltpu.SemaphoreType.DMA((4 + fars,)),
            pltpu.SemaphoreType.DMA((4 + fars,)),
        ],
        compiler_params=pltpu.CompilerParams(
            collective_id=0, has_side_effects=True, vmem_limit_bytes=56 * 1024 * 1024
        ),
        name="fused",
    )(
        view(particles),
        view(projections),
        labels,
        turn_y,
        turn_x,
        weight[None, :],
        weight[None, :] * ctf,
        weight[None, :] * ctf * ctf,
        cos_t,
        sin_t,
    )
    kept = half_rows - 8
    posterior = posterior[:, :, :kept].reshape(2, local_count, cands, -1)
    posterior = jnp.transpose(posterior, (1, 2, 0, 3)).reshape(local_count, cands, -1)
    return posterior, log_total[:, 0]


def fused_fits(particles, projections, tile_list):
    tile_count = lax.axis_size("tile")
    local_count, _, band_width = particles.shape
    return (
        lax.axis_size("shell") == 2
        and tile_count & (tile_count - 1) == 0
        and tile_count * local_count == 4 * LANES
        and band_width % (BOX * tile_count) == 0
        and projections.shape[0] == local_count
        and tile_list.shape[1] % 2 == 0
    )


def per_device(particles, projections, noise_weight, tile_list, ori_start, shifts, defocus_bin):
    plan = fused_plan if fused_fits(particles, projections, tile_list) else slot_plan
    return plan(
        particles, projections, noise_weight, tile_list, ori_start, shifts, defocus_bin
    )


def solution(mesh):
    in_specs = (
        P("tile", None, "shell"),
        P("tile", None, "shell"),
        P("shell"),
        P("tile", None),
        P("tile", None),
        P("tile", None),
        P("tile"),
    )
    out_specs = (P("tile", None, None), P("tile"))
    return jax.shard_map(
        per_device, mesh=mesh, in_specs=in_specs, out_specs=out_specs, check_vma=False
    )
```

```python
import functools
import math

import jax
import jax.numpy as jnp
from jax import lax
from jax.experimental import pallas as pl
from jax.experimental.pallas import tpu as pltpu
from jax.sharding import PartitionSpec as P

BOX = 256
NBIN = 16
TSIDE = 3


wave_length = 0.0197
aberration = 27000000.0
amplitude = 0.1
b_factor = 20.0
defocus_base = 5000.0
defocus_step = 500.0


def frequencies(first_index, span_count):
    flat_index = first_index + jnp.arange(span_count, dtype=jnp.int32)
    freq_x = flat_index // BOX
    freq_y = flat_index % BOX - BOX // 2
    return (freq_x, freq_y)


def ctf_table(freq_x, freq_y, bins_count):
    scaled_x = freq_x.astype(jnp.float32) / BOX
    scaled_y = freq_y.astype(jnp.float32) / BOX
    radius_sq = scaled_x * scaled_x + scaled_y * scaled_y
    defocus = defocus_base + defocus_step * jnp.arange(bins_count, dtype=jnp.float32)[:, None]
    aberr_phase = (
        math.pi * wave_length * defocus * radius_sq[None, :]
        - 0.5 * math.pi * aberration * wave_length**3 * radius_sq[None, :] ** 2
    )
    envelope = jnp.exp(-0.25 * b_factor * radius_sq)[None, :]
    return (
        -(math.sqrt(1.0 - amplitude**2) * jnp.sin(aberr_phase) + amplitude * jnp.cos(aberr_phase))
        * envelope
    )


def rotation(freq_x, freq_y, mult_x, mult_y):
    phase_turns = jnp.mod(freq_x * mult_x + freq_y * mult_y, BOX)
    angles = phase_turns.astype(jnp.float32) * (2.0 * math.pi / BOX)
    return (jnp.cos(angles), jnp.sin(angles))


def pick_rows(bin_index, lookup):
    one_hot = (bin_index[:, None] == jnp.arange(lookup.shape[0], dtype=jnp.int32)[None, :]).astype(
        jnp.float32
    )
    return jnp.dot(
        one_hot, lookup, precision=lax.Precision.HIGHEST, preferred_element_type=jnp.float32
    )


def prepare(particles, weight, ctf_rows, shifts, freq_x, freq_y):
    values = particles.astype(jnp.float32)
    real_part = values[:, 0]
    imag_part = values[:, 1]
    cosine, sine_value = rotation(freq_x[None, :], freq_y[None, :], shifts[:, 0:1], shifts[:, 1:2])
    moved_real = real_part * cosine + imag_part * sine_value
    moved_imag = imag_part * cosine - real_part * sine_value
    factor = weight[None, :] * ctf_rows
    weighted = jnp.stack([factor * moved_real, factor * moved_imag], axis=1).astype(jnp.bfloat16)
    energy = jnp.sum(weight[None, :] * (real_part * real_part + imag_part * imag_part), axis=1)
    return (weighted, energy)


def shifted_tables(projections, freq_x, freq_y):
    offsets = jnp.arange(TSIDE, dtype=jnp.int32) - TSIDE // 2
    mult_x = jnp.repeat(offsets, TSIDE)[:, None]
    mult_y = jnp.tile(offsets, TSIDE)[:, None]
    cosine, sine_value = rotation(freq_x[None, :], freq_y[None, :], mult_x, mult_y)
    cosine = cosine[:, None, :]
    sine_value = sine_value[:, None, :]
    proj_real = projections[:, 0].astype(jnp.float32)[None, :, :]
    proj_imag = projections[:, 1].astype(jnp.float32)[None, :, :]
    moved_real = proj_real * cosine - proj_imag * sine_value
    moved_imag = proj_imag * cosine + proj_real * sine_value
    stacked = jnp.stack([moved_real, moved_imag], axis=2).astype(jnp.bfloat16)
    return stacked.reshape(TSIDE * TSIDE * projections.shape[0], -1)


def slot_scores(slot_rows, bin_index, projections, weight, ctf, freq_x, freq_y):
    orient_count = projections.shape[0]
    lookup = shifted_tables(projections, freq_x, freq_y)
    cross_term = lax.dot_general(
        slot_rows, lookup, (((1,), (1,)), ((), ())), preferred_element_type=jnp.float32
    )
    cross_term = cross_term.reshape(slot_rows.shape[0], TSIDE * TSIDE, orient_count)
    proj_values = projections.astype(jnp.float32)
    magnitude = proj_values[:, 0] * proj_values[:, 0] + proj_values[:, 1] * proj_values[:, 1]
    weighted_ctf = weight[None, :] * ctf * ctf
    power = lax.dot_general(
        weighted_ctf,
        magnitude,
        (((1,), (1,)), ((), ())),
        precision=lax.Precision.HIGHEST,
        preferred_element_type=jnp.float32,
    )
    power_rows = pick_rows(bin_index, power)
    return cross_term - 0.5 * power_rows[:, None, :]


def window(scores, starts, orient_count):
    orient_index = jnp.mod(
        starts[:, None] + jnp.arange(orient_count // 2, dtype=jnp.int32)[None, :], orient_count
    )
    return jnp.take_along_axis(scores, orient_index[:, None, :], axis=2)


def slot_layout(tile_ids, tile_count, capacity):
    positions = jnp.arange(tile_ids.shape[0], dtype=jnp.int32)
    earlier_same = (tile_ids[:, None] == tile_ids[None, :]) & (
        positions[None, :] < positions[:, None]
    )
    slot_rank = jnp.sum(earlier_same.astype(jnp.int32), axis=1)
    slot_index = tile_ids * capacity + slot_rank
    matches = slot_index[None, :] == jnp.arange(tile_count * capacity, dtype=jnp.int32)[:, None]
    slot_owner = jnp.sum(jnp.where(matches, positions[None, :] + 1, 0), axis=1) - 1
    return (slot_index, slot_owner)


def finish(scores, energy_sum):
    scored = scores - 0.5 * energy_sum[:, None, None]
    row_peak = jnp.max(scored, axis=(1, 2))
    log_total = row_peak + jnp.log(jnp.sum(jnp.exp(scored - row_peak[:, None, None]), axis=(1, 2)))
    posterior = jnp.exp(scored - log_total[:, None, None])
    return (posterior, log_total)


def slot_plan(particles, projections, noise_weight, tile_list, ori_start, shifts, defocus_bin):
    tile_count = lax.axis_size("tile")
    band_index = lax.axis_index("shell")
    local_count = particles.shape[0]
    window_count = tile_list.shape[1]
    band_width = particles.shape[2]
    orient_count = projections.shape[0]
    capacity = max(2, (2 * local_count * window_count + tile_count - 1) // tile_count)
    freq_x, freq_y = frequencies(band_index * band_width, band_width)
    ctf = ctf_table(freq_x, freq_y, NBIN)
    weighted, energy = prepare(
        particles, noise_weight, pick_rows(defocus_bin, ctf), shifts, freq_x, freq_y
    )
    weighted = weighted.reshape(local_count, 2 * band_width)
    slot_index, slot_owner = slot_layout(tile_list.reshape(-1), tile_count, capacity)
    occupied = slot_owner >= 0
    item_index = jnp.maximum(slot_owner, 0)
    particle = item_index // window_count
    starts_flat = ori_start.reshape(-1)
    send_rows = jnp.where(
        occupied[:, None], jnp.take(weighted, particle, axis=0), jnp.zeros((), jnp.bfloat16)
    )
    send_rows = send_rows.reshape(tile_count, capacity, 2 * band_width)
    send_labels = jnp.stack(
        [jnp.take(defocus_bin, particle), jnp.take(starts_flat, item_index)], axis=1
    )
    send_labels = send_labels.astype(jnp.bfloat16).reshape(tile_count, capacity, 2)
    payload = lax.all_to_all(send_rows, "tile", split_axis=0, concat_axis=0, tiled=True)
    labels = lax.all_to_all(send_labels, "tile", split_axis=0, concat_axis=0, tiled=True)
    source_count = payload.shape[0]
    slot_count = payload.shape[1]
    slot_rows = payload.reshape(source_count * slot_count, payload.shape[2])
    label_ints = labels.reshape(source_count * slot_count, 2).astype(jnp.int32)
    partial_value = slot_scores(
        slot_rows, label_ints[:, 0], projections, noise_weight, ctf, freq_x, freq_y
    )
    partial_value = partial_value.reshape(
        source_count, slot_count, partial_value.shape[1], partial_value.shape[2]
    )
    returned = lax.all_to_all(partial_value, "tile", split_axis=0, concat_axis=0, tiled=True)
    candidates = returned.shape[2]
    returned = jnp.take(
        returned.reshape(tile_count * capacity, candidates, returned.shape[3]), slot_index, axis=0
    )
    returned = window(returned, starts_flat, orient_count)
    kept = returned.shape[2]
    returned = returned.reshape(local_count, window_count, candidates, kept)
    scores = jnp.transpose(returned, (0, 2, 1, 3)).reshape(
        local_count, candidates, window_count * kept
    )
    scores, energy_sum = lax.psum((scores, energy), "shell")
    return finish(scores, energy_sum)


SHIFT_MAX = 8
HIGH = lax.Precision.HIGHEST


def round_up(value, step):
    return (value + step - 1) // step * step


LANES = 128
MESH = pl.DeviceIdType.MESH


def flip(index, turn, count):
    result = index
    step = 1
    while step < count:
        result = result + step * (turn // step % 2) * (1 - 2 * (index // step % 2))
        step *= 2
    return result


def slot_of(order, fars):
    late = (order // 4 + fars - 1) // fars
    rest = late * (order - 4)
    far = late * (fars - 1 - rest % (fars - 1))
    near = late * (rest // (fars - 1)) + (1 - late) * order
    return far, near


def offset_of(order, fars):
    far, near = slot_of(order, fars)
    return far * 4 + near


def place_of(order, fars):
    far, near = slot_of(order, fars)
    return (near % 2 * 2 + near // 2) * fars + far


def turn_pair(phase):
    angle = (phase & (BOX - 1)).astype(jnp.float32) * (2.0 * math.pi / BOX)
    return jnp.cos(angle), jnp.sin(angle)


def fused_kernel(
    part_ref,
    proj_ref,
    noise_ref,
    tiles_ref,
    starts_ref,
    shifts_ref,
    bins_ref,
    post_ref,
    log_ref,
    label_row,
    label_ref,
    weight_ref,
    turn_y_ref,
    turn_x_ref,
    ctf_ref,
    ctf_sq_ref,
    cos_ref,
    sin_ref,
    part_in,
    proj_in,
    label_in,
    hot,
    wave_y,
    wave_x,
    factor,
    weighted,
    square_sum,
    plain,
    magnitude,
    moved,
    sums,
    core_in,
    side_in,
    far_out,
    far_in,
    pair_out,
    pair_in,
    own_sems,
    send_sems,
    recv_sems,
    back_send,
    back_recv,
):
    tile_count, rows, lines, _ = part_in.shape
    fars = tile_count // 4
    orients = proj_in.shape[1]
    kept = orients // 2
    cands = TSIDE * TSIDE
    middle = cands // 2
    windows = tiles_ref.shape[0]
    chunks = weight_ref.shape[0]
    width = chunks * LANES
    band_rows = width // BOX
    count = weighted.shape[0]
    half_windows = windows // 2
    used = cands * half_windows * kept
    me = lax.axis_index("tile")
    band = lax.axis_index("shell")
    other = 1 - band
    core_peer = flip(me, 1, tile_count)
    side_peer = flip(me, 2, tile_count)

    barrier = pltpu.get_barrier_semaphore()
    peers = [(flip(me, offset, tile_count), band) for offset in range(1, tile_count)]
    peers += [(me, other), (side_peer, other)]
    for peer in peers:
        pl.semaphore_signal(barrier, inc=1, device_id=peer, device_id_type=MESH)
    label_row[...] = jnp.zeros_like(label_row)
    first = 0
    for ref in (tiles_ref, starts_ref, shifts_ref, bins_ref):
        label_row[first : first + ref.shape[0], :rows] = ref[...].astype(jnp.float32)
        first += ref.shape[0]
    for far in range(fars):
        moved_row = pltpu.roll(label_row[...], far * rows, 1) if far else label_row[...]
        label_ref[far] = moved_row.astype(jnp.bfloat16)
    pl.semaphore_wait(barrier, len(peers))

    def remote(source, target, send, recv, peer):
        return pltpu.make_async_remote_copy(
            src_ref=source,
            dst_ref=target,
            send_sem=send,
            recv_sem=recv,
            device_id=peer,
            device_id_type=MESH,
        )

    def piece(ref, tile):
        return ref.at[:, pl.ds(pl.multiple_of(tile * lines, lines), lines), :]

    sent = []
    own_copies = []
    for kind, (source, target) in enumerate(
        ((label_ref, label_in), (part_ref, part_in), (proj_ref, proj_in))
    ):
        if kind:
            copy = pltpu.make_async_copy(piece(source, me), target.at[0], own_sems.at[kind - 1])
            copy.start()
            own_copies.append(copy)
        for order in range(1, tile_count):
            tile = flip(me, offset_of(order, fars), tile_count)
            block = piece(source, tile) if kind else source.at[place_of(order, fars) % fars]
            copy = remote(
                block,
                target.at[order],
                send_sems.at[kind, order],
                recv_sems.at[kind, order],
                (tile, band),
            )
            copy.start()
            sent.append(copy)

    def arrived(kind, target, order):
        remote(
            target.at[order],
            target.at[order],
            send_sems.at[kind, order],
            recv_sems.at[kind, order],
            (core_peer, band),
        ).wait_recv()

    noise = pltpu.make_async_copy(
        noise_ref.at[pl.ds(pl.multiple_of(me * chunks, chunks), chunks), :],
        weight_ref,
        own_sems.at[2],
    )
    noise.start()
    own_copies.append(noise)

    sums[...] = jnp.zeros_like(sums)
    first_line = (band * tile_count + me) * band_rows
    steps = turn_y_ref.shape[0]
    shape = (steps, BOX)
    step = lax.broadcasted_iota(jnp.int32, shape, 0) - SHIFT_MAX
    freq = lax.broadcasted_iota(jnp.int32, shape, 1) - BOX // 2
    cosine, sine_value = turn_pair(step * freq)
    turn_y_ref[:, :BOX] = cosine
    turn_y_ref[:, BOX:] = sine_value
    shape = (steps, LANES)
    step = lax.broadcasted_iota(jnp.int32, shape, 0) - SHIFT_MAX
    line = lax.broadcasted_iota(jnp.int32, shape, 1)
    swap = line >= band_rows
    cosine, sine_value = turn_pair(step * (first_line + jnp.where(swap, line - band_rows, line)))
    turn_x_ref[...] = jnp.where(swap, sine_value, cosine)
    shape = (cos_ref.shape[0], width)
    cand = lax.broadcasted_iota(jnp.int32, shape, 0)
    flat = lax.broadcasted_iota(jnp.int32, shape, 1)
    mult_x = jnp.zeros(shape, jnp.int32)
    for turn in range(1, TSIDE):
        mult_x = mult_x + (cand >= turn * TSIDE).astype(jnp.int32)
    mult_y = cand - TSIDE * mult_x - TSIDE // 2
    mult_x = mult_x - TSIDE // 2
    freq_x = first_line + (flat >> (BOX.bit_length() - 1))
    freq_y = (flat & (BOX - 1)) - BOX // 2
    cosine, sine_value = turn_pair(freq_x * mult_x + freq_y * mult_y)
    cos_ref[...] = cosine
    sin_ref[...] = sine_value
    for copy in own_copies:
        copy.wait()
    shape = (NBIN, LANES)
    defocus_bin = lax.broadcasted_iota(jnp.int32, shape, 0).astype(jnp.float32)
    defocus = defocus_base + defocus_step * defocus_bin
    for chunk in range(chunks):
        line, side = divmod(chunk, BOX // LANES)
        lane = lax.broadcasted_iota(jnp.int32, shape, 1) + (side * LANES - BOX // 2)
        scaled_x = (first_line + line).astype(jnp.float32) / BOX
        scaled_y = lane.astype(jnp.float32) / BOX
        radius_sq = scaled_x * scaled_x + scaled_y * scaled_y
        aberr_phase = (
            math.pi * wave_length * defocus * radius_sq
            - 0.5 * math.pi * aberration * wave_length**3 * radius_sq**2
        )
        envelope = jnp.exp(-0.25 * b_factor * radius_sq)
        ctf = -(
            math.sqrt(1.0 - amplitude**2) * jnp.sin(aberr_phase) + amplitude * jnp.cos(aberr_phase)
        )
        ctf = ctf * envelope
        columns = slice(chunk * LANES, (chunk + 1) * LANES)
        ctf_ref[:, columns] = weight_ref[chunk : chunk + 1, :] * ctf
        ctf_sq_ref[:, columns] = weight_ref[chunk : chunk + 1, :] * ctf * ctf

    label_in[0] = label_ref[0]
    for order in range(1, tile_count):
        arrived(0, label_in, order)
    groups = [jnp.zeros(label_in.shape[1:], jnp.float32)] * 4
    for order in range(tile_count):
        group = place_of(order, fars) // fars
        groups[group] = groups[group] + label_in[order].astype(jnp.float32)
    labels = jnp.concatenate(groups, axis=1)
    tiles = [labels[j : j + 1] for j in range(windows)]
    starts = [labels[windows + j : windows + j + 1] for j in range(windows)]
    shift_x = labels[2 * windows : 2 * windows + 1]
    shift_y = labels[2 * windows + 1 : 2 * windows + 2]
    bins = labels[2 * windows + 2 : 2 * windows + 3]

    def one_hot(row, table_rows, base):
        index = lax.broadcasted_iota(jnp.int32, (table_rows, count), 0).astype(jnp.float32)
        return (index == row + base).astype(jnp.float32)

    def pick(one_hots, table):
        return lax.dot_general(
            one_hots,
            table,
            (((0,), (0,)), ((), ())),
            precision=HIGH,
            preferred_element_type=jnp.float32,
        )

    hot[...] = one_hot(bins, NBIN, 0.0)
    wave_y[...] = pick(one_hot(shift_y, steps, float(SHIFT_MAX)), turn_y_ref[...])
    wave_x[...] = pick(one_hot(shift_x, steps, float(SHIFT_MAX)), turn_x_ref[...])
    factor[...] = pick(hot[...], ctf_ref[...])

    def unpack(value):
        plain[...] = value.reshape(rows * lines, LANES).astype(jnp.float32)

    def parts_of(chunk):
        real_part = plain[pl.ds(2 * chunk, rows, stride=lines), :]
        imag_part = plain[pl.ds(2 * chunk + 1, rows, stride=lines), :]
        return real_part, imag_part

    def weigh(order, carry):
        @pl.when(order > 0)
        def _():
            arrived(1, part_in, order)

        unpack(part_in[order])
        first = pl.multiple_of(place_of(order, fars) * rows, rows)
        span = pl.ds(first, rows)
        energy = jnp.zeros((rows, LANES), jnp.float32)
        for chunk in range(chunks):
            line, side = divmod(chunk, BOX // LANES)
            real_part, imag_part = parts_of(chunk)
            cos_y = wave_y[span, side * LANES : (side + 1) * LANES]
            sin_y = wave_y[span, BOX + side * LANES : BOX + (side + 1) * LANES]
            cos_x = wave_x[span, line : line + 1]
            sin_x = wave_x[span, band_rows + line : band_rows + line + 1]
            cosine = cos_x * cos_y - sin_x * sin_y
            sine_value = sin_x * cos_y + cos_x * sin_y
            columns = slice(chunk * LANES, (chunk + 1) * LANES)
            scale = factor[span, columns]
            weighted[span, columns] = (
                scale * (real_part * cosine + imag_part * sine_value)
            ).astype(jnp.bfloat16)
            weighted[span, width + chunk * LANES : width + (chunk + 1) * LANES] = (
                scale * (imag_part * cosine - real_part * sine_value)
            ).astype(jnp.bfloat16)
            square = real_part * real_part + imag_part * imag_part
            energy += weight_ref[chunk : chunk + 1, :] * square
        square_sum[span, :] = energy
        return carry

    lax.fori_loop(0, tile_count, weigh, 0)
    energy = lax.dot_general(
        jnp.ones((8, LANES), jnp.float32),
        square_sum[...],
        (((1,), (1,)), ((), ())),
        precision=HIGH,
        preferred_element_type=jnp.float32,
    )
    for half in range(2):
        sums[half, used : used + 8, :] = energy

    def score(order, carry):
        @pl.when(order > 0)
        def _():
            arrived(2, proj_in, order)

        unpack(proj_in[order])
        for chunk in range(chunks):
            columns = slice(chunk * LANES, (chunk + 1) * LANES)
            real_part, imag_part = parts_of(chunk)
            magnitude[:, columns] = real_part * real_part + imag_part * imag_part

            def put(cand, real_value, imag_value):
                span = slice(cand * orients, (cand + 1) * orients)
                moved[span, columns] = real_value.astype(jnp.bfloat16)
                moved[span, width + chunk * LANES : width + (chunk + 1) * LANES] = (
                    imag_value.astype(jnp.bfloat16)
                )

            put(middle, real_part, imag_part)
            for cand in range(middle):
                cosine = cos_ref[cand : cand + 1, columns]
                sine_value = sin_ref[cand : cand + 1, columns]
                real_cos = real_part * cosine
                imag_sin = imag_part * sine_value
                imag_cos = imag_part * cosine
                real_sin = real_part * sine_value
                put(cand, real_cos - imag_sin, imag_cos + real_sin)
                put(cands - 1 - cand, real_cos + imag_sin, imag_cos - real_sin)
        power = lax.dot_general(
            magnitude[...],
            ctf_sq_ref[...],
            (((1,), (1,)), ((), ())),
            precision=HIGH,
            preferred_element_type=jnp.float32,
        )
        half_power = 0.5 * jnp.dot(
            power, hot[...], precision=HIGH, preferred_element_type=jnp.float32
        )
        cross = lax.dot_general(
            moved[...],
            weighted[...],
            (((1,), (1,)), ((), ())),
            preferred_element_type=jnp.float32,
        )
        tile = flip(me, offset_of(order, fars), tile_count).astype(jnp.float32)
        named = [row == tile for row in tiles]
        start = jnp.zeros_like(starts[0])
        for j in range(windows):
            start = jnp.where(named[j], starts[j], start)
        start = start.astype(jnp.int32)
        for cand in range(cands):
            value = cross[cand * orients : (cand + 1) * orients] - half_power
            bit = orients // 2
            while bit:
                turned = pltpu.roll(value, orients - bit, 0)
                value = jnp.where((start & bit) != 0, turned, value)
                bit //= 2
            value = value[:kept]
            for j in range(windows):
                half, place = divmod(j, half_windows)
                first = (cand * half_windows + place) * kept
                span = slice(first, first + kept)
                sums[half, span, :] = jnp.where(named[j], value, sums[half, span, :])
        return carry

    lax.fori_loop(0, tile_count, score, 0)

    near = count // 2
    quarter = count // 4
    copy = remote(
        sums.at[:, :, pl.ds(near, near)],
        core_in,
        back_send.at[0],
        back_recv.at[0],
        (core_peer, band),
    )
    copy.start()
    sent.append(copy)
    copy.wait_recv()
    sums[:, :, :near] = sums[:, :, :near] + core_in[...]

    copies = []
    for way, (half, lane, peer) in enumerate(
        (
            (other, quarter, (side_peer, other)),
            (other, 0, (me, other)),
            (band, quarter, (side_peer, band)),
        )
    ):
        copy = remote(
            sums.at[half, :, pl.ds(lane, quarter)],
            side_in.at[way],
            back_send.at[1 + way],
            back_recv.at[1 + way],
            peer,
        )
        copy.start()
        copies.append(copy)
    total = sums[band, :, :quarter]
    for way, copy in enumerate(copies):
        copy.wait_recv()
        total = total + side_in[way]
    sent += copies
    spare = far_out.shape[1] - total.shape[0]
    total = jnp.concatenate([total, jnp.zeros((spare, quarter), jnp.float32)], axis=0)
    far_out[...] = total.T

    copies = []
    for far in range(1, fars):
        copy = remote(
            far_out.at[pl.ds(far * rows, rows), :],
            far_in.at[far],
            back_send.at[3 + far],
            back_recv.at[3 + far],
            (flip(me, 4 * far, tile_count), band),
        )
        copy.start()
        copies.append(copy)
    total = far_out[:rows, :]
    for far, copy in enumerate(copies):
        copy.wait_recv()
        total = total + far_in[1 + far]
    sent += copies
    pair_out[...] = total
    copy = remote(
        pair_out, pair_in, back_send.at[3 + fars], back_recv.at[3 + fars], (me, other)
    )
    copy.start()
    sent.append(copy)
    inside = lax.broadcasted_iota(jnp.int32, total.shape, 1) < used
    low = jnp.full_like(total, -jnp.inf)
    energy = total[:, used : used + 1]
    own = jnp.where(inside, total, low)
    own_peak = jnp.max(own, axis=1, keepdims=True)
    copy.wait_recv()
    theirs = jnp.where(inside, pair_in[...], low)
    peak = jnp.maximum(own_peak, jnp.max(theirs, axis=1, keepdims=True))
    mass = jnp.sum(jnp.exp(own - peak), axis=1, keepdims=True)
    mass += jnp.sum(jnp.exp(theirs - peak), axis=1, keepdims=True)
    log_total = peak + jnp.log(mass)
    own = jnp.exp(own - log_total)
    theirs = jnp.exp(theirs - log_total)
    low = jnp.where(band == 0, own, theirs)
    high = jnp.where(band == 0, theirs, own)
    span = half_windows * kept
    for cand in range(cands):
        columns = slice(cand * span, (cand + 1) * span)
        post_ref[cand] = jnp.concatenate([low[:, columns], high[:, columns]], axis=1)
    evidence = jnp.broadcast_to(log_total - 0.5 * energy, (rows, LANES))
    log_ref[...] = evidence.T[:1, :]
    for copy in sent:
        copy.wait_send()


def fused_plan(particles, projections, noise_weight, tile_list, ori_start, shifts, defocus_bin):
    tile_count = lax.axis_size("tile")
    local_count, pair, band_width = particles.shape
    orients = projections.shape[0]
    windows = tile_list.shape[1]
    width = band_width // tile_count
    count = local_count * tile_count
    cands = TSIDE * TSIDE
    fars = tile_count // 4
    half_rows = cands * (windows // 2) * (orients // 2) + 8
    columns = round_up(half_rows, LANES)
    piece = width // LANES * pair

    label_rows = round_up(2 * windows + shifts.shape[1] + 1, 16)
    steps = round_up(2 * SHIFT_MAX + 1, 8)
    half_cands = round_up(cands // 2, 8)

    def view(values):
        rows = values.shape[0]
        blocks = values.reshape(rows, pair, band_width // LANES, LANES)
        return jnp.transpose(blocks, (0, 2, 1, 3)).reshape(rows, -1, LANES)

    far_space = pl.BlockSpec(memory_space=pl.ANY)
    near_space = pl.BlockSpec(memory_space=pltpu.VMEM)
    posterior, log_total = pl.pallas_call(
        fused_kernel,
        in_specs=[far_space] * 3 + [near_space] * 4,
        out_specs=[near_space] * 2,
        out_shape=[
            jax.ShapeDtypeStruct((cands, local_count, windows * (orients // 2)), jnp.float32),
            jax.ShapeDtypeStruct((1, local_count), jnp.float32),
        ],
        scratch_shapes=[
            pltpu.VMEM((label_rows, LANES), jnp.float32),
            pltpu.VMEM((fars, label_rows, LANES), jnp.bfloat16),
            pltpu.VMEM((width // LANES, LANES), jnp.float32),
            pltpu.VMEM((steps, 2 * BOX), jnp.float32),
            pltpu.VMEM((steps, LANES), jnp.float32),
            pltpu.VMEM((NBIN, width), jnp.float32),
            pltpu.VMEM((NBIN, width), jnp.float32),
            pltpu.VMEM((half_cands, width), jnp.float32),
            pltpu.VMEM((half_cands, width), jnp.float32),
            pltpu.VMEM((tile_count, local_count, piece, LANES), jnp.bfloat16),
            pltpu.VMEM((tile_count, orients, piece, LANES), jnp.bfloat16),
            pltpu.VMEM((tile_count, label_rows, LANES), jnp.bfloat16),
            pltpu.VMEM((NBIN, count), jnp.float32),
            pltpu.VMEM((count, 2 * BOX), jnp.float32),
            pltpu.VMEM((count, LANES), jnp.float32),
            pltpu.VMEM((count, width), jnp.float32),
            pltpu.VMEM((count, pair * width), jnp.bfloat16),
            pltpu.VMEM((count, LANES), jnp.float32),
            pltpu.VMEM((local_count * piece, LANES), jnp.float32),
            pltpu.VMEM((orients, width), jnp.float32),
            pltpu.VMEM((cands * orients, pair * width), jnp.bfloat16),
            pltpu.VMEM((2, half_rows, count), jnp.float32),
            pltpu.VMEM((2, half_rows, count // 2), jnp.float32),
            pltpu.VMEM((3, half_rows, count // 4), jnp.float32),
            pltpu.VMEM((count // 4, columns), jnp.float32),
            pltpu.VMEM((fars, local_count, columns), jnp.float32),
            pltpu.VMEM((local_count, columns), jnp.float32),
            pltpu.VMEM((local_count, columns), jnp.float32),
            pltpu.SemaphoreType.DMA((3,)),
            pltpu.SemaphoreType.DMA((3, tile_count)),
            pltpu.SemaphoreType.DMA((3, tile_count)),
            pltpu.SemaphoreType.DMA((4 + fars,)),
            pltpu.SemaphoreType.DMA((4 + fars,)),
        ],
        compiler_params=pltpu.CompilerParams(
            collective_id=0, has_side_effects=True, vmem_limit_bytes=56 * 1024 * 1024
        ),
        name="fused",
    )(
        view(particles),
        view(projections),
        noise_weight.reshape(-1, LANES),
        tile_list.T,
        ori_start.T,
        shifts.T,
        defocus_bin[None, :],
    )
    return jnp.transpose(posterior, (1, 0, 2)), log_total[0]


def fused_fits(particles, projections, tile_list):
    tile_count = lax.axis_size("tile")
    local_count, _, band_width = particles.shape
    return (
        lax.axis_size("shell") == 2
        and tile_count & (tile_count - 1) == 0
        and tile_count * local_count == 4 * LANES
        and band_width % (BOX * tile_count) == 0
        and projections.shape[0] == local_count
        and tile_list.shape[1] % 2 == 0
    )


def per_device(particles, projections, noise_weight, tile_list, ori_start, shifts, defocus_bin):
    plan = fused_plan if fused_fits(particles, projections, tile_list) else slot_plan
    return plan(
        particles, projections, noise_weight, tile_list, ori_start, shifts, defocus_bin
    )


def solution(mesh):
    in_specs = (
        P("tile", None, "shell"),
        P("tile", None, "shell"),
        P("shell"),
        P("tile", None),
        P("tile", None),
        P("tile", None),
        P("tile"),
    )
    out_specs = (P("tile", None, None), P("tile"))
    return jax.shard_map(
        per_device, mesh=mesh, in_specs=in_specs, out_specs=out_specs, check_vma=False
    )
```

```python
import functools
import math

import jax
import jax.numpy as jnp
from jax import lax
from jax.experimental import pallas as pl
from jax.experimental.pallas import tpu as pltpu
from jax.sharding import PartitionSpec as P

BOX = 256
NBIN = 16
TSIDE = 3


wave_length = 0.0197
aberration = 27000000.0
amplitude = 0.1
b_factor = 20.0
defocus_base = 5000.0
defocus_step = 500.0


def frequencies(first_index, span_count):
    flat_index = first_index + jnp.arange(span_count, dtype=jnp.int32)
    freq_x = flat_index // BOX
    freq_y = flat_index % BOX - BOX // 2
    return (freq_x, freq_y)


def ctf_table(freq_x, freq_y, bins_count):
    scaled_x = freq_x.astype(jnp.float32) / BOX
    scaled_y = freq_y.astype(jnp.float32) / BOX
    radius_sq = scaled_x * scaled_x + scaled_y * scaled_y
    defocus = defocus_base + defocus_step * jnp.arange(bins_count, dtype=jnp.float32)[:, None]
    aberr_phase = (
        math.pi * wave_length * defocus * radius_sq[None, :]
        - 0.5 * math.pi * aberration * wave_length**3 * radius_sq[None, :] ** 2
    )
    envelope = jnp.exp(-0.25 * b_factor * radius_sq)[None, :]
    return (
        -(math.sqrt(1.0 - amplitude**2) * jnp.sin(aberr_phase) + amplitude * jnp.cos(aberr_phase))
        * envelope
    )


def rotation(freq_x, freq_y, mult_x, mult_y):
    phase_turns = jnp.mod(freq_x * mult_x + freq_y * mult_y, BOX)
    angles = phase_turns.astype(jnp.float32) * (2.0 * math.pi / BOX)
    return (jnp.cos(angles), jnp.sin(angles))


def pick_rows(bin_index, lookup):
    one_hot = (bin_index[:, None] == jnp.arange(lookup.shape[0], dtype=jnp.int32)[None, :]).astype(
        jnp.float32
    )
    return jnp.dot(
        one_hot, lookup, precision=lax.Precision.HIGHEST, preferred_element_type=jnp.float32
    )


def prepare(particles, weight, ctf_rows, shifts, freq_x, freq_y):
    values = particles.astype(jnp.float32)
    real_part = values[:, 0]
    imag_part = values[:, 1]
    cosine, sine_value = rotation(freq_x[None, :], freq_y[None, :], shifts[:, 0:1], shifts[:, 1:2])
    moved_real = real_part * cosine + imag_part * sine_value
    moved_imag = imag_part * cosine - real_part * sine_value
    factor = weight[None, :] * ctf_rows
    weighted = jnp.stack([factor * moved_real, factor * moved_imag], axis=1).astype(jnp.bfloat16)
    energy = jnp.sum(weight[None, :] * (real_part * real_part + imag_part * imag_part), axis=1)
    return (weighted, energy)


def shifted_tables(projections, freq_x, freq_y):
    offsets = jnp.arange(TSIDE, dtype=jnp.int32) - TSIDE // 2
    mult_x = jnp.repeat(offsets, TSIDE)[:, None]
    mult_y = jnp.tile(offsets, TSIDE)[:, None]
    cosine, sine_value = rotation(freq_x[None, :], freq_y[None, :], mult_x, mult_y)
    cosine = cosine[:, None, :]
    sine_value = sine_value[:, None, :]
    proj_real = projections[:, 0].astype(jnp.float32)[None, :, :]
    proj_imag = projections[:, 1].astype(jnp.float32)[None, :, :]
    moved_real = proj_real * cosine - proj_imag * sine_value
    moved_imag = proj_imag * cosine + proj_real * sine_value
    stacked = jnp.stack([moved_real, moved_imag], axis=2).astype(jnp.bfloat16)
    return stacked.reshape(TSIDE * TSIDE * projections.shape[0], -1)


def slot_scores(slot_rows, bin_index, projections, weight, ctf, freq_x, freq_y):
    orient_count = projections.shape[0]
    lookup = shifted_tables(projections, freq_x, freq_y)
    cross_term = lax.dot_general(
        slot_rows, lookup, (((1,), (1,)), ((), ())), preferred_element_type=jnp.float32
    )
    cross_term = cross_term.reshape(slot_rows.shape[0], TSIDE * TSIDE, orient_count)
    proj_values = projections.astype(jnp.float32)
    magnitude = proj_values[:, 0] * proj_values[:, 0] + proj_values[:, 1] * proj_values[:, 1]
    weighted_ctf = weight[None, :] * ctf * ctf
    power = lax.dot_general(
        weighted_ctf,
        magnitude,
        (((1,), (1,)), ((), ())),
        precision=lax.Precision.HIGHEST,
        preferred_element_type=jnp.float32,
    )
    power_rows = pick_rows(bin_index, power)
    return cross_term - 0.5 * power_rows[:, None, :]


def window(scores, starts, orient_count):
    orient_index = jnp.mod(
        starts[:, None] + jnp.arange(orient_count // 2, dtype=jnp.int32)[None, :], orient_count
    )
    return jnp.take_along_axis(scores, orient_index[:, None, :], axis=2)


def slot_layout(tile_ids, tile_count, capacity):
    positions = jnp.arange(tile_ids.shape[0], dtype=jnp.int32)
    earlier_same = (tile_ids[:, None] == tile_ids[None, :]) & (
        positions[None, :] < positions[:, None]
    )
    slot_rank = jnp.sum(earlier_same.astype(jnp.int32), axis=1)
    slot_index = tile_ids * capacity + slot_rank
    matches = slot_index[None, :] == jnp.arange(tile_count * capacity, dtype=jnp.int32)[:, None]
    slot_owner = jnp.sum(jnp.where(matches, positions[None, :] + 1, 0), axis=1) - 1
    return (slot_index, slot_owner)


def finish(scores, energy_sum):
    scored = scores - 0.5 * energy_sum[:, None, None]
    row_peak = jnp.max(scored, axis=(1, 2))
    log_total = row_peak + jnp.log(jnp.sum(jnp.exp(scored - row_peak[:, None, None]), axis=(1, 2)))
    posterior = jnp.exp(scored - log_total[:, None, None])
    return (posterior, log_total)


def slot_plan(particles, projections, noise_weight, tile_list, ori_start, shifts, defocus_bin):
    tile_count = lax.axis_size("tile")
    band_index = lax.axis_index("shell")
    local_count = particles.shape[0]
    window_count = tile_list.shape[1]
    band_width = particles.shape[2]
    orient_count = projections.shape[0]
    capacity = max(2, (2 * local_count * window_count + tile_count - 1) // tile_count)
    freq_x, freq_y = frequencies(band_index * band_width, band_width)
    ctf = ctf_table(freq_x, freq_y, NBIN)
    weighted, energy = prepare(
        particles, noise_weight, pick_rows(defocus_bin, ctf), shifts, freq_x, freq_y
    )
    weighted = weighted.reshape(local_count, 2 * band_width)
    slot_index, slot_owner = slot_layout(tile_list.reshape(-1), tile_count, capacity)
    occupied = slot_owner >= 0
    item_index = jnp.maximum(slot_owner, 0)
    particle = item_index // window_count
    starts_flat = ori_start.reshape(-1)
    send_rows = jnp.where(
        occupied[:, None], jnp.take(weighted, particle, axis=0), jnp.zeros((), jnp.bfloat16)
    )
    send_rows = send_rows.reshape(tile_count, capacity, 2 * band_width)
    send_labels = jnp.stack(
        [jnp.take(defocus_bin, particle), jnp.take(starts_flat, item_index)], axis=1
    )
    send_labels = send_labels.astype(jnp.bfloat16).reshape(tile_count, capacity, 2)
    payload = lax.all_to_all(send_rows, "tile", split_axis=0, concat_axis=0, tiled=True)
    labels = lax.all_to_all(send_labels, "tile", split_axis=0, concat_axis=0, tiled=True)
    source_count = payload.shape[0]
    slot_count = payload.shape[1]
    slot_rows = payload.reshape(source_count * slot_count, payload.shape[2])
    label_ints = labels.reshape(source_count * slot_count, 2).astype(jnp.int32)
    partial_value = slot_scores(
        slot_rows, label_ints[:, 0], projections, noise_weight, ctf, freq_x, freq_y
    )
    partial_value = partial_value.reshape(
        source_count, slot_count, partial_value.shape[1], partial_value.shape[2]
    )
    returned = lax.all_to_all(partial_value, "tile", split_axis=0, concat_axis=0, tiled=True)
    candidates = returned.shape[2]
    returned = jnp.take(
        returned.reshape(tile_count * capacity, candidates, returned.shape[3]), slot_index, axis=0
    )
    returned = window(returned, starts_flat, orient_count)
    kept = returned.shape[2]
    returned = returned.reshape(local_count, window_count, candidates, kept)
    scores = jnp.transpose(returned, (0, 2, 1, 3)).reshape(
        local_count, candidates, window_count * kept
    )
    scores, energy_sum = lax.psum((scores, energy), "shell")
    return finish(scores, energy_sum)


SHIFT_MAX = 8
HIGH = lax.Precision.HIGHEST


def round_up(value, step):
    return (value + step - 1) // step * step


LANES = 128
CODE_TOP = 32000.0
MESH = pl.DeviceIdType.MESH


def flip(index, turn, count):
    result = index
    step = 1
    while step < count:
        result = result + step * (turn // step % 2) * (1 - 2 * (index // step % 2))
        step *= 2
    return result


def slot_of(order, fars):
    late = (order // 4 + fars - 1) // fars
    rest = late * (order - 4)
    far = late * (fars - 1 - rest % (fars - 1))
    near = late * (rest // (fars - 1)) + (1 - late) * order
    return far, near


def offset_of(order, fars):
    far, near = slot_of(order, fars)
    return far * 4 + near


def place_of(order, fars):
    far, near = slot_of(order, fars)
    return (near % 2 * 2 + near // 2) * fars + far


def turn_pair(phase):
    angle = (phase & (BOX - 1)).astype(jnp.float32) * (2.0 * math.pi / BOX)
    return jnp.cos(angle), jnp.sin(angle)


def fused_kernel(
    part_ref,
    proj_ref,
    noise_ref,
    tiles_ref,
    starts_ref,
    shifts_ref,
    bins_ref,
    low_ref,
    high_ref,
    label_row,
    label_ref,
    weight_ref,
    turn_y_ref,
    turn_x_ref,
    ctf_ref,
    ctf_sq_ref,
    cos_ref,
    sin_ref,
    part_in,
    proj_in,
    label_in,
    hot,
    wave_y,
    wave_x,
    factor,
    weighted,
    local_part,
    local_noise,
    noise_rows,
    square_sum,
    plain,
    magnitude,
    moved,
    sums,
    core_in,
    side_out,
    side_in,
    far_sum,
    far_out,
    far_in,
    pair_out,
    pair_in,
    own_sems,
    send_sems,
    recv_sems,
    back_send,
    back_recv,
):
    tile_count, rows, lines, _ = part_in.shape
    fars = tile_count // 4
    orients = proj_in.shape[1]
    kept = orients // 2
    cands = TSIDE * TSIDE
    middle = cands // 2
    windows = tiles_ref.shape[0]
    chunks = weight_ref.shape[0]
    width = chunks * LANES
    band_rows = width // BOX
    count = weighted.shape[0]
    half_windows = windows // 2
    used = cands * half_windows * kept
    me = lax.axis_index("tile")
    band = lax.axis_index("shell")
    other = 1 - band
    core_peer = flip(me, 1, tile_count)
    side_peer = flip(me, 2, tile_count)

    barrier = pltpu.get_barrier_semaphore()
    peers = [(flip(me, offset, tile_count), band) for offset in range(1, tile_count)]
    peers += [(me, other), (side_peer, other)]
    for peer in peers:
        pl.semaphore_signal(barrier, inc=1, device_id=peer, device_id_type=MESH)
    label_row[...] = jnp.zeros_like(label_row)
    first = 0
    for ref in (tiles_ref, starts_ref, shifts_ref, bins_ref):
        label_row[first : first + ref.shape[0], :rows] = ref[...].astype(jnp.float32)
        first += ref.shape[0]
    for far in range(fars):
        moved_row = pltpu.roll(label_row[...], far * rows, 1) if far else label_row[...]
        label_ref[far] = moved_row.astype(jnp.bfloat16)
    pl.semaphore_wait(barrier, len(peers))

    def remote(source, target, send, recv, peer):
        return pltpu.make_async_remote_copy(
            src_ref=source,
            dst_ref=target,
            send_sem=send,
            recv_sem=recv,
            device_id=peer,
            device_id_type=MESH,
        )

    def piece(ref, tile):
        return ref.at[:, pl.ds(pl.multiple_of(tile * lines, lines), lines), :]

    sent = []
    own_copies = []
    for kind, (source, target) in enumerate(
        ((label_ref, label_in), (part_ref, part_in), (proj_ref, proj_in))
    ):
        if kind:
            copy = pltpu.make_async_copy(piece(source, me), target.at[0], own_sems.at[kind - 1])
            copy.start()
            own_copies.append(copy)
        for order in range(1, tile_count):
            tile = flip(me, offset_of(order, fars), tile_count)
            block = piece(source, tile) if kind else source.at[place_of(order, fars) % fars]
            copy = remote(
                block,
                target.at[order],
                send_sems.at[kind, order],
                recv_sems.at[kind, order],
                (tile, band),
            )
            copy.start()
            sent.append(copy)

    def arrived(kind, target, order):
        remote(
            target.at[order],
            target.at[order],
            send_sems.at[kind, order],
            recv_sems.at[kind, order],
            (core_peer, band),
        ).wait_recv()

    noise = pltpu.make_async_copy(
        noise_ref.at[pl.ds(pl.multiple_of(me * chunks, chunks), chunks), :],
        weight_ref,
        own_sems.at[2],
    )
    noise.start()
    own_copies.append(noise)
    local_copies = [
        pltpu.make_async_copy(part_ref, local_part, own_sems.at[3]),
        pltpu.make_async_copy(noise_ref, local_noise, own_sems.at[4]),
    ]
    for copy in local_copies:
        copy.start()

    sums[...] = jnp.zeros_like(sums)
    first_line = (band * tile_count + me) * band_rows
    steps = turn_y_ref.shape[0]
    shape = (steps, BOX)
    step = lax.broadcasted_iota(jnp.int32, shape, 0) - SHIFT_MAX
    freq = lax.broadcasted_iota(jnp.int32, shape, 1) - BOX // 2
    cosine, sine_value = turn_pair(step * freq)
    turn_y_ref[:, :BOX] = cosine
    turn_y_ref[:, BOX:] = sine_value
    shape = (steps, LANES)
    step = lax.broadcasted_iota(jnp.int32, shape, 0) - SHIFT_MAX
    line = lax.broadcasted_iota(jnp.int32, shape, 1)
    swap = line >= band_rows
    cosine, sine_value = turn_pair(step * (first_line + jnp.where(swap, line - band_rows, line)))
    turn_x_ref[...] = jnp.where(swap, sine_value, cosine)
    shape = (cos_ref.shape[0], width)
    cand = lax.broadcasted_iota(jnp.int32, shape, 0)
    flat = lax.broadcasted_iota(jnp.int32, shape, 1)
    mult_x = jnp.zeros(shape, jnp.int32)
    for turn in range(1, TSIDE):
        mult_x = mult_x + (cand >= turn * TSIDE).astype(jnp.int32)
    mult_y = cand - TSIDE * mult_x - TSIDE // 2
    mult_x = mult_x - TSIDE // 2
    freq_x = first_line + (flat >> (BOX.bit_length() - 1))
    freq_y = (flat & (BOX - 1)) - BOX // 2
    cosine, sine_value = turn_pair(freq_x * mult_x + freq_y * mult_y)
    cos_ref[...] = cosine
    sin_ref[...] = sine_value
    for copy in own_copies:
        copy.wait()
    shape = (NBIN, LANES)
    defocus_bin = lax.broadcasted_iota(jnp.int32, shape, 0).astype(jnp.float32)
    defocus = defocus_base + defocus_step * defocus_bin
    for chunk in range(chunks):
        line, side = divmod(chunk, BOX // LANES)
        lane = lax.broadcasted_iota(jnp.int32, shape, 1) + (side * LANES - BOX // 2)
        scaled_x = (first_line + line).astype(jnp.float32) / BOX
        scaled_y = lane.astype(jnp.float32) / BOX
        radius_sq = scaled_x * scaled_x + scaled_y * scaled_y
        aberr_phase = (
            math.pi * wave_length * defocus * radius_sq
            - 0.5 * math.pi * aberration * wave_length**3 * radius_sq**2
        )
        envelope = jnp.exp(-0.25 * b_factor * radius_sq)
        ctf = -(
            math.sqrt(1.0 - amplitude**2) * jnp.sin(aberr_phase) + amplitude * jnp.cos(aberr_phase)
        )
        ctf = ctf * envelope
        columns = slice(chunk * LANES, (chunk + 1) * LANES)
        ctf_ref[:, columns] = weight_ref[chunk : chunk + 1, :] * ctf
        ctf_sq_ref[:, columns] = weight_ref[chunk : chunk + 1, :] * ctf * ctf

    label_in[0] = label_ref[0]
    for order in range(1, tile_count):
        arrived(0, label_in, order)
    groups = [jnp.zeros(label_in.shape[1:], jnp.float32)] * 4
    for order in range(tile_count):
        group = place_of(order, fars) // fars
        groups[group] = groups[group] + label_in[order].astype(jnp.float32)
    labels = jnp.concatenate(groups, axis=1)
    tiles = [labels[j : j + 1] for j in range(windows)]
    starts = [labels[windows + j : windows + j + 1] for j in range(windows)]
    shift_x = labels[2 * windows : 2 * windows + 1]
    shift_y = labels[2 * windows + 1 : 2 * windows + 2]
    bins = labels[2 * windows + 2 : 2 * windows + 3]

    def one_hot(row, table_rows, base):
        index = lax.broadcasted_iota(jnp.int32, (table_rows, count), 0).astype(jnp.float32)
        return (index == row + base).astype(jnp.float32)

    def pick(one_hots, table):
        return lax.dot_general(
            one_hots,
            table,
            (((0,), (0,)), ((), ())),
            precision=HIGH,
            preferred_element_type=jnp.float32,
        )

    hot[...] = one_hot(bins, NBIN, 0.0)
    wave_y[...] = pick(one_hot(shift_y, steps, float(SHIFT_MAX)), turn_y_ref[...])
    wave_x[...] = pick(one_hot(shift_x, steps, float(SHIFT_MAX)), turn_x_ref[...])
    factor[...] = pick(hot[...], ctf_ref[...])

    for copy in local_copies:
        copy.wait()
    pairs = local_noise.shape[0]
    for part in range(2):
        noise_rows[pl.ds(part, pairs, stride=2), :] = local_noise[...]

    def square(particle, carry):
        total = jnp.zeros((8, LANES), jnp.float32)
        for first in range(0, 2 * pairs, 16):
            value = local_part[particle, first : first + 16, :].astype(jnp.float32)
            value = value * value * noise_rows[first : first + 16, :]
            total = total + value[:8] + value[8:]
        square_sum[pl.ds(particle, 1), :] = jnp.sum(total, axis=0, keepdims=True)
        return carry

    lax.fori_loop(0, rows, square, 0)

    def unpack(value):
        plain[...] = value.reshape(rows * lines, LANES).astype(jnp.float32)

    def parts_of(chunk):
        real_part = plain[pl.ds(2 * chunk, rows, stride=lines), :]
        imag_part = plain[pl.ds(2 * chunk + 1, rows, stride=lines), :]
        return real_part, imag_part

    def weigh(order, carry):
        @pl.when(order > 0)
        def _():
            arrived(1, part_in, order)

        unpack(part_in[order])
        first = pl.multiple_of(place_of(order, fars) * rows, rows)
        span = pl.ds(first, rows)
        for chunk in range(chunks):
            line, side = divmod(chunk, BOX // LANES)
            real_part, imag_part = parts_of(chunk)
            cos_y = wave_y[span, side * LANES : (side + 1) * LANES]
            sin_y = wave_y[span, BOX + side * LANES : BOX + (side + 1) * LANES]
            cos_x = wave_x[span, line : line + 1]
            sin_x = wave_x[span, band_rows + line : band_rows + line + 1]
            cosine = cos_x * cos_y - sin_x * sin_y
            sine_value = sin_x * cos_y + cos_x * sin_y
            columns = slice(chunk * LANES, (chunk + 1) * LANES)
            scale = factor[span, columns]
            weighted[span, columns] = (
                scale * (real_part * cosine + imag_part * sine_value)
            ).astype(jnp.bfloat16)
            weighted[span, width + chunk * LANES : width + (chunk + 1) * LANES] = (
                scale * (imag_part * cosine - real_part * sine_value)
            ).astype(jnp.bfloat16)
        return carry

    lax.fori_loop(0, tile_count, weigh, 0)

    def score(order, carry):
        @pl.when(order > 0)
        def _():
            arrived(2, proj_in, order)

        unpack(proj_in[order])
        for chunk in range(chunks):
            columns = slice(chunk * LANES, (chunk + 1) * LANES)
            real_part, imag_part = parts_of(chunk)
            magnitude[:, columns] = real_part * real_part + imag_part * imag_part

            def put(cand, real_value, imag_value):
                span = slice(cand * orients, (cand + 1) * orients)
                moved[span, columns] = real_value.astype(jnp.bfloat16)
                moved[span, width + chunk * LANES : width + (chunk + 1) * LANES] = (
                    imag_value.astype(jnp.bfloat16)
                )

            put(middle, real_part, imag_part)
            for cand in range(middle):
                cosine = cos_ref[cand : cand + 1, columns]
                sine_value = sin_ref[cand : cand + 1, columns]
                real_cos = real_part * cosine
                imag_sin = imag_part * sine_value
                imag_cos = imag_part * cosine
                real_sin = real_part * sine_value
                put(cand, real_cos - imag_sin, imag_cos + real_sin)
                put(cands - 1 - cand, real_cos + imag_sin, imag_cos - real_sin)
        power = lax.dot_general(
            magnitude[...],
            ctf_sq_ref[...],
            (((1,), (1,)), ((), ())),
            precision=HIGH,
            preferred_element_type=jnp.float32,
        )
        half_power = 0.5 * jnp.dot(
            power, hot[...], precision=HIGH, preferred_element_type=jnp.float32
        )
        cross = lax.dot_general(
            moved[...],
            weighted[...],
            (((1,), (1,)), ((), ())),
            preferred_element_type=jnp.float32,
        )
        tile = flip(me, offset_of(order, fars), tile_count).astype(jnp.float32)
        named = [row == tile for row in tiles]
        start = jnp.zeros_like(starts[0])
        for j in range(windows):
            start = jnp.where(named[j], starts[j], start)
        start = start.astype(jnp.int32)
        for cand in range(cands):
            value = cross[cand * orients : (cand + 1) * orients] - half_power
            bit = orients // 2
            while bit:
                turned = pltpu.roll(value, orients - bit, 0)
                value = jnp.where((start & bit) != 0, turned, value)
                bit //= 2
            value = value[:kept]
            for j in range(windows):
                half, place = divmod(j, half_windows)
                first = (cand * half_windows + place) * kept
                span = slice(first, first + kept)
                sums[half, span, :] = jnp.where(named[j], value, sums[half, span, :])
        return carry

    lax.fori_loop(0, tile_count, score, 0)

    near = count // 2
    quarter = count // 4
    copy = remote(
        sums.at[:, :, pl.ds(near, near)],
        core_in,
        back_send.at[0],
        back_recv.at[0],
        (core_peer, band),
    )
    copy.start()
    sent.append(copy)
    copy.wait_recv()
    sums[:, :, :near] = sums[:, :, :near] + core_in[...]

    def scale_of(peak):
        return jnp.ceil(jnp.log2(jnp.maximum(peak, 1e-30)))

    def coded(value, scale):
        return jnp.round(value * (CODE_TOP * jnp.exp2(-scale))).astype(jnp.int32)

    def plain_of(code, scale):
        return code.astype(jnp.float32) * (jnp.exp2(scale) / CODE_TOP)

    whole = sums[:, :, :near]
    peak = jnp.max(jnp.max(jnp.abs(whole), axis=0), axis=0, keepdims=True)
    scale = scale_of(peak)
    scale_rows = side_out.shape[1] - used
    for half in range(2):
        side_out[half, :used, :] = coded(whole[half], scale).astype(jnp.int16)
        side_out[half, used:, :] = (
            jnp.broadcast_to(scale, (scale_rows, near)).astype(jnp.int32).astype(jnp.int16)
        )
    copies = []
    for way, (half, lane, peer) in enumerate(
        (
            (other, quarter, (side_peer, other)),
            (other, 0, (me, other)),
            (band, quarter, (side_peer, band)),
        )
    ):
        copy = remote(
            side_out.at[half, :, pl.ds(lane, quarter)],
            side_in.at[way],
            back_send.at[1 + way],
            back_recv.at[1 + way],
            peer,
        )
        copy.start()
        copies.append(copy)
    total = sums[band, :, :quarter]
    for way, copy in enumerate(copies):
        copy.wait_recv()
        code = side_in[way].astype(jnp.int32)
        total = total + plain_of(code[:used], code[used : used + 1].astype(jnp.float32))
    sent += copies
    columns = far_out.shape[1]
    total = jnp.concatenate([total, jnp.zeros((columns - used, quarter), jnp.float32)], axis=0)
    total = total.T
    far_sum[...] = total
    scale = scale_of(jnp.max(jnp.abs(total), axis=1, keepdims=True))
    column = lax.broadcasted_iota(jnp.int32, total.shape, 1)
    code = coded(total, scale)
    far_out[...] = jnp.where(column >= used, scale.astype(jnp.int32), code).astype(jnp.int16)

    copies = []
    for far in range(1, fars):
        copy = remote(
            far_out.at[pl.ds(far * rows, rows), :],
            far_in.at[far],
            back_send.at[3 + far],
            back_recv.at[3 + far],
            (flip(me, 4 * far, tile_count), band),
        )
        copy.start()
        copies.append(copy)
    energy = jnp.sum(square_sum[...], axis=1, keepdims=True)
    total = far_sum[:rows, :]
    for far, copy in enumerate(copies):
        copy.wait_recv()
        code = far_in[1 + far].astype(jnp.int32)
        total = total + plain_of(code, code[:, used : used + 1].astype(jnp.float32))
    sent += copies
    column = lax.broadcasted_iota(jnp.int32, total.shape, 1)
    total = jnp.where(column >= used, energy, total)
    pair_out[...] = total
    copy = remote(
        pair_out, pair_in, back_send.at[3 + fars], back_recv.at[3 + fars], (me, other)
    )
    copy.start()
    sent.append(copy)
    copy.wait_recv()
    theirs = pair_in[...]
    low_ref[...] = jnp.where(band == 0, total, theirs)
    high_ref[...] = jnp.where(band == 0, theirs, total)
    for copy in sent:
        copy.wait_send()


def settle_kernel(low_ref, high_ref, post_ref, log_ref):
    cands, rows, span = post_ref.shape
    used = cands * span // 2
    low = low_ref[...]
    high = high_ref[...]
    inside = lax.broadcasted_iota(jnp.int32, low.shape, 1) < used
    least = jnp.full_like(low, -jnp.inf)
    energy = low[:, used : used + 1] + high[:, used : used + 1]
    low = jnp.where(inside, low, least)
    high = jnp.where(inside, high, least)
    peak = jnp.max(jnp.maximum(low, high), axis=1, keepdims=True)
    mass = jnp.sum(jnp.exp(low - peak) + jnp.exp(high - peak), axis=1, keepdims=True)
    log_total = peak + jnp.log(mass)
    low = jnp.exp(low - log_total)
    high = jnp.exp(high - log_total)
    half = span // 2
    for cand in range(cands):
        columns = slice(cand * half, (cand + 1) * half)
        post_ref[cand] = jnp.concatenate([low[:, columns], high[:, columns]], axis=1)
    evidence = jnp.broadcast_to(log_total - 0.5 * energy, (rows, LANES))
    log_ref[...] = evidence.T[:1, :]


def fused_plan(particles, projections, noise_weight, tile_list, ori_start, shifts, defocus_bin):
    tile_count = lax.axis_size("tile")
    local_count, pair, band_width = particles.shape
    orients = projections.shape[0]
    windows = tile_list.shape[1]
    width = band_width // tile_count
    count = local_count * tile_count
    cands = TSIDE * TSIDE
    fars = tile_count // 4
    half_rows = cands * (windows // 2) * (orients // 2)
    coded_rows = half_rows + 16
    columns = round_up(half_rows + 1, LANES)
    piece = width // LANES * pair

    label_rows = round_up(2 * windows + shifts.shape[1] + 1, 16)
    steps = round_up(2 * SHIFT_MAX + 1, 8)
    half_cands = round_up(cands // 2, 8)

    def view(values):
        rows = values.shape[0]
        blocks = values.reshape(rows, pair, band_width // LANES, LANES)
        return jnp.transpose(blocks, (0, 2, 1, 3)).reshape(rows, -1, LANES)

    far_space = pl.BlockSpec(memory_space=pl.ANY)
    near_space = pl.BlockSpec(memory_space=pltpu.VMEM)
    low, high = pl.pallas_call(
        fused_kernel,
        in_specs=[far_space] * 3 + [near_space] * 4,
        out_specs=[near_space] * 2,
        out_shape=[pltpu.VMEM((local_count, columns), jnp.float32)] * 2,
        scratch_shapes=[
            pltpu.VMEM((label_rows, LANES), jnp.float32),
            pltpu.VMEM((fars, label_rows, LANES), jnp.bfloat16),
            pltpu.VMEM((width // LANES, LANES), jnp.float32),
            pltpu.VMEM((steps, 2 * BOX), jnp.float32),
            pltpu.VMEM((steps, LANES), jnp.float32),
            pltpu.VMEM((NBIN, width), jnp.float32),
            pltpu.VMEM((NBIN, width), jnp.float32),
            pltpu.VMEM((half_cands, width), jnp.float32),
            pltpu.VMEM((half_cands, width), jnp.float32),
            pltpu.VMEM((tile_count, local_count, piece, LANES), jnp.bfloat16),
            pltpu.VMEM((tile_count, orients, piece, LANES), jnp.bfloat16),
            pltpu.VMEM((tile_count, label_rows, LANES), jnp.bfloat16),
            pltpu.VMEM((NBIN, count), jnp.float32),
            pltpu.VMEM((count, 2 * BOX), jnp.float32),
            pltpu.VMEM((count, LANES), jnp.float32),
            pltpu.VMEM((count, width), jnp.float32),
            pltpu.VMEM((count, pair * width), jnp.bfloat16),
            pltpu.VMEM((local_count, band_width // LANES * pair, LANES), jnp.bfloat16),
            pltpu.VMEM((band_width // LANES, LANES), jnp.float32),
            pltpu.VMEM((band_width // LANES * pair, LANES), jnp.float32),
            pltpu.VMEM((local_count, LANES), jnp.float32),
            pltpu.VMEM((local_count * piece, LANES), jnp.float32),
            pltpu.VMEM((orients, width), jnp.float32),
            pltpu.VMEM((cands * orients, pair * width), jnp.bfloat16),
            pltpu.VMEM((2, half_rows, count), jnp.float32),
            pltpu.VMEM((2, half_rows, count // 2), jnp.float32),
            pltpu.VMEM((2, coded_rows, count // 2), jnp.int16),
            pltpu.VMEM((3, coded_rows, count // 4), jnp.int16),
            pltpu.VMEM((count // 4, columns), jnp.float32),
            pltpu.VMEM((count // 4, columns), jnp.int16),
            pltpu.VMEM((fars, local_count, columns), jnp.int16),
            pltpu.VMEM((local_count, columns), jnp.float32),
            pltpu.VMEM((local_count, columns), jnp.float32),
            pltpu.SemaphoreType.DMA((5,)),
            pltpu.SemaphoreType.DMA((3, tile_count)),
            pltpu.SemaphoreType.DMA((3, tile_count)),
            pltpu.SemaphoreType.DMA((4 + fars,)),
            pltpu.SemaphoreType.DMA((4 + fars,)),
        ],
        compiler_params=pltpu.CompilerParams(
            collective_id=0, has_side_effects=True, vmem_limit_bytes=56 * 1024 * 1024
        ),
        name="fused",
    )(
        view(particles),
        view(projections),
        noise_weight.reshape(-1, LANES),
        tile_list.T,
        ori_start.T,
        shifts.T,
        defocus_bin[None, :],
    )
    posterior, log_total = pl.pallas_call(
        settle_kernel,
        in_specs=[near_space] * 2,
        out_specs=[near_space] * 2,
        out_shape=[
            jax.ShapeDtypeStruct((cands, local_count, windows * (orients // 2)), jnp.float32),
            jax.ShapeDtypeStruct((1, local_count), jnp.float32),
        ],
        compiler_params=pltpu.CompilerParams(vmem_limit_bytes=4 * 1024 * 1024),
        name="settle",
    )(low, high)
    return jnp.transpose(posterior, (1, 0, 2)), log_total[0]


def fused_fits(particles, projections, tile_list):
    tile_count = lax.axis_size("tile")
    local_count, _, band_width = particles.shape
    return (
        lax.axis_size("shell") == 2
        and tile_count & (tile_count - 1) == 0
        and tile_count * local_count == 4 * LANES
        and band_width % (BOX * tile_count) == 0
        and projections.shape[0] == local_count
        and tile_list.shape[1] % 2 == 0
    )


def per_device(particles, projections, noise_weight, tile_list, ori_start, shifts, defocus_bin):
    plan = fused_plan if fused_fits(particles, projections, tile_list) else slot_plan
    return plan(
        particles, projections, noise_weight, tile_list, ori_start, shifts, defocus_bin
    )


def solution(mesh):
    in_specs = (
        P("tile", None, "shell"),
        P("tile", None, "shell"),
        P("shell"),
        P("tile", None),
        P("tile", None),
        P("tile", None),
        P("tile"),
    )
    out_specs = (P("tile", None, None), P("tile"))
    return jax.shard_map(
        per_device, mesh=mesh, in_specs=in_specs, out_specs=out_specs, check_vma=False
    )
```

```python
import functools
import math

import jax
import jax.numpy as jnp
from jax import lax
from jax.experimental import pallas as pl
from jax.experimental.pallas import tpu as pltpu
from jax.sharding import PartitionSpec as P

BOX = 256
NBIN = 16
TSIDE = 3


wave_length = 0.0197
aberration = 27000000.0
amplitude = 0.1
b_factor = 20.0
defocus_base = 5000.0
defocus_step = 500.0


def frequencies(first_index, span_count):
    flat_index = first_index + jnp.arange(span_count, dtype=jnp.int32)
    freq_x = flat_index // BOX
    freq_y = flat_index % BOX - BOX // 2
    return (freq_x, freq_y)


def ctf_table(freq_x, freq_y, bins_count):
    scaled_x = freq_x.astype(jnp.float32) / BOX
    scaled_y = freq_y.astype(jnp.float32) / BOX
    radius_sq = scaled_x * scaled_x + scaled_y * scaled_y
    defocus = defocus_base + defocus_step * jnp.arange(bins_count, dtype=jnp.float32)[:, None]
    aberr_phase = (
        math.pi * wave_length * defocus * radius_sq[None, :]
        - 0.5 * math.pi * aberration * wave_length**3 * radius_sq[None, :] ** 2
    )
    envelope = jnp.exp(-0.25 * b_factor * radius_sq)[None, :]
    return (
        -(math.sqrt(1.0 - amplitude**2) * jnp.sin(aberr_phase) + amplitude * jnp.cos(aberr_phase))
        * envelope
    )


def rotation(freq_x, freq_y, mult_x, mult_y):
    phase_turns = jnp.mod(freq_x * mult_x + freq_y * mult_y, BOX)
    angles = phase_turns.astype(jnp.float32) * (2.0 * math.pi / BOX)
    return (jnp.cos(angles), jnp.sin(angles))


def pick_rows(bin_index, lookup):
    one_hot = (bin_index[:, None] == jnp.arange(lookup.shape[0], dtype=jnp.int32)[None, :]).astype(
        jnp.float32
    )
    return jnp.dot(
        one_hot, lookup, precision=lax.Precision.HIGHEST, preferred_element_type=jnp.float32
    )


def prepare(particles, weight, ctf_rows, shifts, freq_x, freq_y):
    values = particles.astype(jnp.float32)
    real_part = values[:, 0]
    imag_part = values[:, 1]
    cosine, sine_value = rotation(freq_x[None, :], freq_y[None, :], shifts[:, 0:1], shifts[:, 1:2])
    moved_real = real_part * cosine + imag_part * sine_value
    moved_imag = imag_part * cosine - real_part * sine_value
    factor = weight[None, :] * ctf_rows
    weighted = jnp.stack([factor * moved_real, factor * moved_imag], axis=1).astype(jnp.bfloat16)
    energy = jnp.sum(weight[None, :] * (real_part * real_part + imag_part * imag_part), axis=1)
    return (weighted, energy)


def shifted_tables(projections, freq_x, freq_y):
    offsets = jnp.arange(TSIDE, dtype=jnp.int32) - TSIDE // 2
    mult_x = jnp.repeat(offsets, TSIDE)[:, None]
    mult_y = jnp.tile(offsets, TSIDE)[:, None]
    cosine, sine_value = rotation(freq_x[None, :], freq_y[None, :], mult_x, mult_y)
    cosine = cosine[:, None, :]
    sine_value = sine_value[:, None, :]
    proj_real = projections[:, 0].astype(jnp.float32)[None, :, :]
    proj_imag = projections[:, 1].astype(jnp.float32)[None, :, :]
    moved_real = proj_real * cosine - proj_imag * sine_value
    moved_imag = proj_imag * cosine + proj_real * sine_value
    stacked = jnp.stack([moved_real, moved_imag], axis=2).astype(jnp.bfloat16)
    return stacked.reshape(TSIDE * TSIDE * projections.shape[0], -1)


def slot_scores(slot_rows, bin_index, projections, weight, ctf, freq_x, freq_y):
    orient_count = projections.shape[0]
    lookup = shifted_tables(projections, freq_x, freq_y)
    cross_term = lax.dot_general(
        slot_rows, lookup, (((1,), (1,)), ((), ())), preferred_element_type=jnp.float32
    )
    cross_term = cross_term.reshape(slot_rows.shape[0], TSIDE * TSIDE, orient_count)
    proj_values = projections.astype(jnp.float32)
    magnitude = proj_values[:, 0] * proj_values[:, 0] + proj_values[:, 1] * proj_values[:, 1]
    weighted_ctf = weight[None, :] * ctf * ctf
    power = lax.dot_general(
        weighted_ctf,
        magnitude,
        (((1,), (1,)), ((), ())),
        precision=lax.Precision.HIGHEST,
        preferred_element_type=jnp.float32,
    )
    power_rows = pick_rows(bin_index, power)
    return cross_term - 0.5 * power_rows[:, None, :]


def window(scores, starts, orient_count):
    orient_index = jnp.mod(
        starts[:, None] + jnp.arange(orient_count // 2, dtype=jnp.int32)[None, :], orient_count
    )
    return jnp.take_along_axis(scores, orient_index[:, None, :], axis=2)


def slot_layout(tile_ids, tile_count, capacity):
    positions = jnp.arange(tile_ids.shape[0], dtype=jnp.int32)
    earlier_same = (tile_ids[:, None] == tile_ids[None, :]) & (
        positions[None, :] < positions[:, None]
    )
    slot_rank = jnp.sum(earlier_same.astype(jnp.int32), axis=1)
    slot_index = tile_ids * capacity + slot_rank
    matches = slot_index[None, :] == jnp.arange(tile_count * capacity, dtype=jnp.int32)[:, None]
    slot_owner = jnp.sum(jnp.where(matches, positions[None, :] + 1, 0), axis=1) - 1
    return (slot_index, slot_owner)


def finish(scores, energy_sum):
    scored = scores - 0.5 * energy_sum[:, None, None]
    row_peak = jnp.max(scored, axis=(1, 2))
    log_total = row_peak + jnp.log(jnp.sum(jnp.exp(scored - row_peak[:, None, None]), axis=(1, 2)))
    posterior = jnp.exp(scored - log_total[:, None, None])
    return (posterior, log_total)


def slot_plan(particles, projections, noise_weight, tile_list, ori_start, shifts, defocus_bin):
    tile_count = lax.axis_size("tile")
    band_index = lax.axis_index("shell")
    local_count = particles.shape[0]
    window_count = tile_list.shape[1]
    band_width = particles.shape[2]
    orient_count = projections.shape[0]
    capacity = max(2, (2 * local_count * window_count + tile_count - 1) // tile_count)
    freq_x, freq_y = frequencies(band_index * band_width, band_width)
    ctf = ctf_table(freq_x, freq_y, NBIN)
    weighted, energy = prepare(
        particles, noise_weight, pick_rows(defocus_bin, ctf), shifts, freq_x, freq_y
    )
    weighted = weighted.reshape(local_count, 2 * band_width)
    slot_index, slot_owner = slot_layout(tile_list.reshape(-1), tile_count, capacity)
    occupied = slot_owner >= 0
    item_index = jnp.maximum(slot_owner, 0)
    particle = item_index // window_count
    starts_flat = ori_start.reshape(-1)
    send_rows = jnp.where(
        occupied[:, None], jnp.take(weighted, particle, axis=0), jnp.zeros((), jnp.bfloat16)
    )
    send_rows = send_rows.reshape(tile_count, capacity, 2 * band_width)
    send_labels = jnp.stack(
        [jnp.take(defocus_bin, particle), jnp.take(starts_flat, item_index)], axis=1
    )
    send_labels = send_labels.astype(jnp.bfloat16).reshape(tile_count, capacity, 2)
    payload = lax.all_to_all(send_rows, "tile", split_axis=0, concat_axis=0, tiled=True)
    labels = lax.all_to_all(send_labels, "tile", split_axis=0, concat_axis=0, tiled=True)
    source_count = payload.shape[0]
    slot_count = payload.shape[1]
    slot_rows = payload.reshape(source_count * slot_count, payload.shape[2])
    label_ints = labels.reshape(source_count * slot_count, 2).astype(jnp.int32)
    partial_value = slot_scores(
        slot_rows, label_ints[:, 0], projections, noise_weight, ctf, freq_x, freq_y
    )
    partial_value = partial_value.reshape(
        source_count, slot_count, partial_value.shape[1], partial_value.shape[2]
    )
    returned = lax.all_to_all(partial_value, "tile", split_axis=0, concat_axis=0, tiled=True)
    candidates = returned.shape[2]
    returned = jnp.take(
        returned.reshape(tile_count * capacity, candidates, returned.shape[3]), slot_index, axis=0
    )
    returned = window(returned, starts_flat, orient_count)
    kept = returned.shape[2]
    returned = returned.reshape(local_count, window_count, candidates, kept)
    scores = jnp.transpose(returned, (0, 2, 1, 3)).reshape(
        local_count, candidates, window_count * kept
    )
    scores, energy_sum = lax.psum((scores, energy), "shell")
    return finish(scores, energy_sum)


SHIFT_MAX = 8
HIGH = lax.Precision.HIGHEST


def round_up(value, step):
    return (value + step - 1) // step * step


LANES = 128
CODE_TOP = 32000.0
MESH = pl.DeviceIdType.MESH


def flip(index, turn, count):
    result = index
    step = 1
    while step < count:
        result = result + step * (turn // step % 2) * (1 - 2 * (index // step % 2))
        step *= 2
    return result


def slot_of(order, fars):
    late = (order // 4 + fars - 1) // fars
    rest = late * (order - 4)
    far = late * (fars - 1 - rest % (fars - 1))
    near = late * (rest // (fars - 1)) + (1 - late) * order
    return far, near


def offset_of(order, fars):
    far, near = slot_of(order, fars)
    return far * 4 + near


def place_of(order, fars):
    far, near = slot_of(order, fars)
    return (near % 2 * 2 + near // 2) * fars + far


def turn_pair(phase):
    angle = (phase & (BOX - 1)).astype(jnp.float32) * (2.0 * math.pi / BOX)
    return jnp.cos(angle), jnp.sin(angle)


def three(value):
    parts = []
    for _ in range(3):
        part = value.astype(jnp.bfloat16)
        value = value - part.astype(jnp.float32)
        parts.append(part)
    return parts


def fused_kernel(
    part_ref,
    proj_ref,
    noise_ref,
    tiles_ref,
    starts_ref,
    shifts_ref,
    bins_ref,
    low_ref,
    high_ref,
    label_row,
    label_ref,
    weight_ref,
    turn_y_ref,
    turn_x_ref,
    ctf_ref,
    power_ref,
    cos_ref,
    sin_ref,
    part_in,
    proj_in,
    label_in,
    hot_parts,
    wave_y,
    wave_x,
    factor,
    weighted,
    local_part,
    local_noise,
    noise_rows,
    square_sum,
    plain,
    magnitude,
    moved,
    sums,
    core_in,
    side_out,
    side_in,
    far_sum,
    far_out,
    far_in,
    pair_out,
    pair_in,
    own_sems,
    send_sems,
    recv_sems,
    back_send,
    back_recv,
    core_send,
    core_recv,
):
    tile_count, rows, lines, _ = part_in.shape
    fars = tile_count // 4
    orients = proj_in.shape[1]
    kept = orients // 2
    cands = TSIDE * TSIDE
    middle = cands // 2
    windows = tiles_ref.shape[0]
    chunks = weight_ref.shape[0]
    width = chunks * LANES
    band_rows = width // BOX
    count = weighted.shape[0]
    half_windows = windows // 2
    used = cands * half_windows * kept
    me = lax.axis_index("tile")
    band = lax.axis_index("shell")
    other = 1 - band
    core_peer = flip(me, 1, tile_count)
    side_peer = flip(me, 2, tile_count)

    barrier = pltpu.get_barrier_semaphore()
    peers = [(flip(me, offset, tile_count), band) for offset in range(1, tile_count)]
    peers += [(me, other), (side_peer, other)]
    for peer in peers:
        pl.semaphore_signal(barrier, inc=1, device_id=peer, device_id_type=MESH)
    label_row[...] = jnp.zeros_like(label_row)
    first = 0
    for ref in (tiles_ref, starts_ref, shifts_ref, bins_ref):
        label_row[first : first + ref.shape[0], :rows] = ref[...].astype(jnp.float32)
        first += ref.shape[0]
    for far in range(fars):
        moved_row = pltpu.roll(label_row[...], far * rows, 1) if far else label_row[...]
        label_ref[far] = moved_row.astype(jnp.bfloat16)
    pl.semaphore_wait(barrier, len(peers))

    def remote(source, target, send, recv, peer):
        return pltpu.make_async_remote_copy(
            src_ref=source,
            dst_ref=target,
            send_sem=send,
            recv_sem=recv,
            device_id=peer,
            device_id_type=MESH,
        )

    def piece(ref, tile):
        return ref.at[:, pl.ds(pl.multiple_of(tile * lines, lines), lines), :]

    sent = []
    own_copies = []
    for kind, (source, target) in enumerate(
        ((label_ref, label_in), (part_ref, part_in), (proj_ref, proj_in))
    ):
        if kind:
            copy = pltpu.make_async_copy(piece(source, me), target.at[0], own_sems.at[kind - 1])
            copy.start()
            own_copies.append(copy)
        for order in range(1, tile_count):
            tile = flip(me, offset_of(order, fars), tile_count)
            block = piece(source, tile) if kind else source.at[place_of(order, fars) % fars]
            copy = remote(
                block,
                target.at[order],
                send_sems.at[kind, order],
                recv_sems.at[kind, order],
                (tile, band),
            )
            copy.start()
            sent.append(copy)

    def arrived(kind, target, order):
        remote(
            target.at[order],
            target.at[order],
            send_sems.at[kind, order],
            recv_sems.at[kind, order],
            (core_peer, band),
        ).wait_recv()

    noise = pltpu.make_async_copy(
        noise_ref.at[pl.ds(pl.multiple_of(me * chunks, chunks), chunks), :],
        weight_ref,
        own_sems.at[2],
    )
    noise.start()
    own_copies.append(noise)
    local_copies = [
        pltpu.make_async_copy(part_ref, local_part, own_sems.at[3]),
        pltpu.make_async_copy(noise_ref, local_noise, own_sems.at[4]),
    ]
    for copy in local_copies:
        copy.start()

    sums[...] = jnp.zeros_like(sums)
    first_line = (band * tile_count + me) * band_rows
    steps = turn_y_ref.shape[0]
    shape = (steps, BOX)
    step = lax.broadcasted_iota(jnp.int32, shape, 0) - SHIFT_MAX
    freq = lax.broadcasted_iota(jnp.int32, shape, 1) - BOX // 2
    cosine, sine_value = turn_pair(step * freq)
    turn_y_ref[:, :BOX] = cosine
    turn_y_ref[:, BOX:] = sine_value
    shape = (steps, LANES)
    step = lax.broadcasted_iota(jnp.int32, shape, 0) - SHIFT_MAX
    line = lax.broadcasted_iota(jnp.int32, shape, 1)
    swap = line >= band_rows
    cosine, sine_value = turn_pair(step * (first_line + jnp.where(swap, line - band_rows, line)))
    turn_x_ref[...] = jnp.where(swap, sine_value, cosine)
    shape = (cos_ref.shape[0], width)
    cand = lax.broadcasted_iota(jnp.int32, shape, 0)
    flat = lax.broadcasted_iota(jnp.int32, shape, 1)
    mult_x = jnp.zeros(shape, jnp.int32)
    for turn in range(1, TSIDE):
        mult_x = mult_x + (cand >= turn * TSIDE).astype(jnp.int32)
    mult_y = cand - TSIDE * mult_x - TSIDE // 2
    mult_x = mult_x - TSIDE // 2
    freq_x = first_line + (flat >> (BOX.bit_length() - 1))
    freq_y = (flat & (BOX - 1)) - BOX // 2
    cosine, sine_value = turn_pair(freq_x * mult_x + freq_y * mult_y)
    cos_ref[...] = cosine
    sin_ref[...] = sine_value
    for copy in own_copies:
        copy.wait()
    shape = (NBIN, LANES)
    defocus_bin = lax.broadcasted_iota(jnp.int32, shape, 0).astype(jnp.float32)
    defocus = defocus_base + defocus_step * defocus_bin
    for chunk in range(chunks):
        line, side = divmod(chunk, BOX // LANES)
        lane = lax.broadcasted_iota(jnp.int32, shape, 1) + (side * LANES - BOX // 2)
        scaled_x = (first_line + line).astype(jnp.float32) / BOX
        scaled_y = lane.astype(jnp.float32) / BOX
        radius_sq = scaled_x * scaled_x + scaled_y * scaled_y
        aberr_phase = (
            math.pi * wave_length * defocus * radius_sq
            - 0.5 * math.pi * aberration * wave_length**3 * radius_sq**2
        )
        envelope = jnp.exp(-0.25 * b_factor * radius_sq)
        ctf = -(
            math.sqrt(1.0 - amplitude**2) * jnp.sin(aberr_phase) + amplitude * jnp.cos(aberr_phase)
        )
        ctf = ctf * envelope
        columns = slice(chunk * LANES, (chunk + 1) * LANES)
        ctf_ref[:, columns] = weight_ref[chunk : chunk + 1, :] * ctf
        for part, value in enumerate(three(0.5 * weight_ref[chunk : chunk + 1, :] * ctf * ctf)):
            power_ref[part * NBIN : (part + 1) * NBIN, columns] = value

    label_in[0] = label_ref[0]
    for order in range(1, tile_count):
        arrived(0, label_in, order)
    groups = [jnp.zeros(label_in.shape[1:], jnp.float32)] * 4
    for order in range(tile_count):
        group = place_of(order, fars) // fars
        groups[group] = groups[group] + label_in[order].astype(jnp.float32)
    labels = jnp.concatenate(groups, axis=1)
    tiles = [labels[j : j + 1] for j in range(windows)]
    starts = [labels[windows + j : windows + j + 1] for j in range(windows)]
    shift_x = labels[2 * windows : 2 * windows + 1]
    shift_y = labels[2 * windows + 1 : 2 * windows + 2]
    bins = labels[2 * windows + 2 : 2 * windows + 3]

    def one_hot(row, table_rows, base):
        index = lax.broadcasted_iota(jnp.int32, (table_rows, count), 0).astype(jnp.float32)
        return (index == row + base).astype(jnp.float32)

    def pick(one_hots, table):
        return lax.dot_general(
            one_hots,
            table,
            (((0,), (0,)), ((), ())),
            precision=HIGH,
            preferred_element_type=jnp.float32,
        )

    hot = one_hot(bins, NBIN, 0.0)
    hot_parts[...] = jnp.concatenate([hot] * 3, axis=0).astype(jnp.bfloat16)
    wave_y[...] = pick(one_hot(shift_y, steps, float(SHIFT_MAX)), turn_y_ref[...])
    wave_x[...] = pick(one_hot(shift_x, steps, float(SHIFT_MAX)), turn_x_ref[...])
    factor[...] = pick(hot, ctf_ref[...])

    for copy in local_copies:
        copy.wait()
    pairs = local_noise.shape[0]
    for part in range(2):
        noise_rows[pl.ds(part, pairs, stride=2), :] = local_noise[...]

    def square(particle, carry):
        total = jnp.zeros((8, LANES), jnp.float32)
        for first in range(0, 2 * pairs, 16):
            value = local_part[particle, first : first + 16, :].astype(jnp.float32)
            value = value * value * noise_rows[first : first + 16, :]
            total = total + value[:8] + value[8:]
        square_sum[pl.ds(particle, 1), :] = jnp.sum(total, axis=0, keepdims=True)
        return carry

    lax.fori_loop(0, rows, square, 0)

    def unpack(value):
        plain[...] = value.reshape(rows * lines, LANES).astype(jnp.float32)

    def parts_of(chunk):
        real_part = plain[pl.ds(2 * chunk, rows, stride=lines), :]
        imag_part = plain[pl.ds(2 * chunk + 1, rows, stride=lines), :]
        return real_part, imag_part

    def weigh(order, carry):
        @pl.when(order > 0)
        def _():
            arrived(1, part_in, order)

        unpack(part_in[order])
        first = pl.multiple_of(place_of(order, fars) * rows, rows)
        span = pl.ds(first, rows)
        for chunk in range(chunks):
            line, side = divmod(chunk, BOX // LANES)
            real_part, imag_part = parts_of(chunk)
            cos_y = wave_y[span, side * LANES : (side + 1) * LANES]
            sin_y = wave_y[span, BOX + side * LANES : BOX + (side + 1) * LANES]
            cos_x = wave_x[span, line : line + 1]
            sin_x = wave_x[span, band_rows + line : band_rows + line + 1]
            cosine = cos_x * cos_y - sin_x * sin_y
            sine_value = sin_x * cos_y + cos_x * sin_y
            columns = slice(chunk * LANES, (chunk + 1) * LANES)
            scale = factor[span, columns]
            weighted[span, columns] = (
                scale * (real_part * cosine + imag_part * sine_value)
            ).astype(jnp.bfloat16)
            weighted[span, width + chunk * LANES : width + (chunk + 1) * LANES] = (
                scale * (imag_part * cosine - real_part * sine_value)
            ).astype(jnp.bfloat16)
        return carry

    lax.fori_loop(0, tile_count, weigh, 0)

    def score(order, carry):
        @pl.when(order > 0)
        def _():
            arrived(2, proj_in, order)

        unpack(proj_in[order])
        for chunk in range(chunks):
            columns = slice(chunk * LANES, (chunk + 1) * LANES)
            real_part, imag_part = parts_of(chunk)
            for part, value in enumerate(three(real_part * real_part + imag_part * imag_part)):
                magnitude[part * orients : (part + 1) * orients, columns] = value

            def put(cand, real_value, imag_value):
                span = slice(cand * orients, (cand + 1) * orients)
                moved[span, columns] = real_value.astype(jnp.bfloat16)
                moved[span, width + chunk * LANES : width + (chunk + 1) * LANES] = (
                    imag_value.astype(jnp.bfloat16)
                )

            put(middle, real_part, imag_part)
            for cand in range(middle):
                cosine = cos_ref[cand : cand + 1, columns]
                sine_value = sin_ref[cand : cand + 1, columns]
                real_cos = real_part * cosine
                imag_sin = imag_part * sine_value
                imag_cos = imag_part * cosine
                real_sin = real_part * sine_value
                put(cand, real_cos - imag_sin, imag_cos + real_sin)
                put(cands - 1 - cand, real_cos + imag_sin, imag_cos - real_sin)
        power = lax.dot_general(
            magnitude[...],
            power_ref[...],
            (((1,), (1,)), ((), ())),
            preferred_element_type=jnp.float32,
        )
        power = power[:orients] + power[orients : 2 * orients] + power[2 * orients :]
        half_power = jnp.dot(
            jnp.concatenate(three(power), axis=0),
            hot_parts[...],
            preferred_element_type=jnp.float32,
        )
        half_power = (
            half_power[:orients] + half_power[orients : 2 * orients] + half_power[2 * orients :]
        )
        cross = lax.dot_general(
            moved[...],
            weighted[...],
            (((1,), (1,)), ((), ())),
            preferred_element_type=jnp.float32,
        )
        tile = flip(me, offset_of(order, fars), tile_count).astype(jnp.float32)
        named = [row == tile for row in tiles]
        start = jnp.zeros_like(starts[0])
        for j in range(windows):
            start = jnp.where(named[j], starts[j], start)
        start = start.astype(jnp.int32)
        for cand in range(cands):
            value = cross[cand * orients : (cand + 1) * orients] - half_power
            bit = orients // 2
            while bit:
                turned = pltpu.roll(value, orients - bit, 0)
                value = jnp.where((start & bit) != 0, turned, value)
                bit //= 2
            value = value[:kept]
            for j in range(windows):
                half, place = divmod(j, half_windows)
                first = (cand * half_windows + place) * kept
                span = slice(first, first + kept)
                sums[half, span, :] = jnp.where(named[j], value, sums[half, span, :])
        return carry

    lax.fori_loop(0, tile_count, score, 0)

    near = count // 2
    quarter = count // 4
    core_copies = []
    for turn, half in enumerate((other, band)):
        copy = remote(
            sums.at[half, :, pl.ds(near, near)],
            core_in.at[half],
            core_send.at[turn],
            core_recv.at[turn],
            (core_peer, band),
        )
        copy.start()
        core_copies.append(copy)
    sent += core_copies

    def scale_of(peak):
        return jnp.ceil(jnp.log2(jnp.maximum(peak, 1e-30)))

    def coded(value, scale):
        return jnp.round(value * (CODE_TOP * jnp.exp2(-scale))).astype(jnp.int32)

    def plain_of(code, scale):
        return code.astype(jnp.float32) * (jnp.exp2(scale) / CODE_TOP)

    scale_rows = side_out.shape[1] - used
    copies = []
    for turn, half in enumerate((other, band)):
        core_copies[turn].wait_recv()
        whole = sums[half, :, :near] + core_in[half]
        sums[half, :, :near] = whole
        scale = scale_of(jnp.max(jnp.abs(whole), axis=0, keepdims=True))
        side_out[half, :used, :] = coded(whole, scale).astype(jnp.int16)
        side_out[half, used:, :] = (
            jnp.broadcast_to(scale, (scale_rows, near)).astype(jnp.int32).astype(jnp.int16)
        )
        ways = ((1, (side_peer, other)), (0, (me, other))) if turn == 0 else ((1, (side_peer, band)),)
        for lane, peer in ways:
            way = len(copies)
            copy = remote(
                side_out.at[half, :, pl.ds(lane * quarter, quarter)],
                side_in.at[way],
                back_send.at[1 + way],
                back_recv.at[1 + way],
                peer,
            )
            copy.start()
            copies.append(copy)
    total = sums[band, :, :quarter]
    for way, copy in enumerate(copies):
        copy.wait_recv()
        code = side_in[way].astype(jnp.int32)
        total = total + plain_of(code[:used], code[used : used + 1].astype(jnp.float32))
    sent += copies
    columns = far_out.shape[1]
    total = jnp.concatenate([total, jnp.zeros((columns - used, quarter), jnp.float32)], axis=0)
    total = total.T
    far_sum[...] = total
    scale = scale_of(jnp.max(jnp.abs(total), axis=1, keepdims=True))
    column = lax.broadcasted_iota(jnp.int32, total.shape, 1)
    code = coded(total, scale)
    far_out[...] = jnp.where(column >= used, scale.astype(jnp.int32), code).astype(jnp.int16)

    copies = []
    for far in range(1, fars):
        copy = remote(
            far_out.at[pl.ds(far * rows, rows), :],
            far_in.at[far],
            back_send.at[3 + far],
            back_recv.at[3 + far],
            (flip(me, 4 * far, tile_count), band),
        )
        copy.start()
        copies.append(copy)
    energy = jnp.sum(square_sum[...], axis=1, keepdims=True)
    total = far_sum[:rows, :]
    for far, copy in enumerate(copies):
        copy.wait_recv()
        code = far_in[1 + far].astype(jnp.int32)
        total = total + plain_of(code, code[:, used : used + 1].astype(jnp.float32))
    sent += copies
    column = lax.broadcasted_iota(jnp.int32, total.shape, 1)
    total = jnp.where(column >= used, energy, total)
    pair_out[...] = total
    copy = remote(
        pair_out, pair_in, back_send.at[3 + fars], back_recv.at[3 + fars], (me, other)
    )
    copy.start()
    sent.append(copy)
    copy.wait_recv()
    theirs = pair_in[...]
    low_ref[...] = jnp.where(band == 0, total, theirs)
    high_ref[...] = jnp.where(band == 0, theirs, total)
    for copy in sent:
        copy.wait_send()


def settle_kernel(low_ref, high_ref, post_ref, log_ref):
    cands, rows, span = post_ref.shape
    used = cands * span // 2
    low = low_ref[...]
    high = high_ref[...]
    inside = lax.broadcasted_iota(jnp.int32, low.shape, 1) < used
    least = jnp.full_like(low, -jnp.inf)
    energy = low[:, used : used + 1] + high[:, used : used + 1]
    low = jnp.where(inside, low, least)
    high = jnp.where(inside, high, least)
    peak = jnp.max(jnp.maximum(low, high), axis=1, keepdims=True)
    mass = jnp.sum(jnp.exp(low - peak) + jnp.exp(high - peak), axis=1, keepdims=True)
    log_total = peak + jnp.log(mass)
    low = jnp.exp(low - log_total)
    high = jnp.exp(high - log_total)
    half = span // 2
    for cand in range(cands):
        columns = slice(cand * half, (cand + 1) * half)
        post_ref[cand] = jnp.concatenate([low[:, columns], high[:, columns]], axis=1)
    evidence = jnp.broadcast_to(log_total - 0.5 * energy, (rows, LANES))
    log_ref[...] = evidence.T[:1, :]


def fused_plan(particles, projections, noise_weight, tile_list, ori_start, shifts, defocus_bin):
    tile_count = lax.axis_size("tile")
    local_count, pair, band_width = particles.shape
    orients = projections.shape[0]
    windows = tile_list.shape[1]
    width = band_width // tile_count
    count = local_count * tile_count
    cands = TSIDE * TSIDE
    fars = tile_count // 4
    half_rows = cands * (windows // 2) * (orients // 2)
    coded_rows = half_rows + 16
    columns = round_up(half_rows + 1, LANES)
    piece = width // LANES * pair

    label_rows = round_up(2 * windows + shifts.shape[1] + 1, 16)
    steps = round_up(2 * SHIFT_MAX + 1, 8)
    half_cands = round_up(cands // 2, 8)

    def view(values):
        rows = values.shape[0]
        blocks = values.reshape(rows, pair, band_width // LANES, LANES)
        return jnp.transpose(blocks, (0, 2, 1, 3)).reshape(rows, -1, LANES)

    far_space = pl.BlockSpec(memory_space=pl.ANY)
    near_space = pl.BlockSpec(memory_space=pltpu.VMEM)
    low, high = pl.pallas_call(
        fused_kernel,
        in_specs=[far_space] * 3 + [near_space] * 4,
        out_specs=[near_space] * 2,
        out_shape=[pltpu.VMEM((local_count, columns), jnp.float32)] * 2,
        scratch_shapes=[
            pltpu.VMEM((label_rows, LANES), jnp.float32),
            pltpu.VMEM((fars, label_rows, LANES), jnp.bfloat16),
            pltpu.VMEM((width // LANES, LANES), jnp.float32),
            pltpu.VMEM((steps, 2 * BOX), jnp.float32),
            pltpu.VMEM((steps, LANES), jnp.float32),
            pltpu.VMEM((NBIN, width), jnp.float32),
            pltpu.VMEM((3 * NBIN, width), jnp.bfloat16),
            pltpu.VMEM((half_cands, width), jnp.float32),
            pltpu.VMEM((half_cands, width), jnp.float32),
            pltpu.VMEM((tile_count, local_count, piece, LANES), jnp.bfloat16),
            pltpu.VMEM((tile_count, orients, piece, LANES), jnp.bfloat16),
            pltpu.VMEM((tile_count, label_rows, LANES), jnp.bfloat16),
            pltpu.VMEM((3 * NBIN, count), jnp.bfloat16),
            pltpu.VMEM((count, 2 * BOX), jnp.float32),
            pltpu.VMEM((count, LANES), jnp.float32),
            pltpu.VMEM((count, width), jnp.float32),
            pltpu.VMEM((count, pair * width), jnp.bfloat16),
            pltpu.VMEM((local_count, band_width // LANES * pair, LANES), jnp.bfloat16),
            pltpu.VMEM((band_width // LANES, LANES), jnp.float32),
            pltpu.VMEM((band_width // LANES * pair, LANES), jnp.float32),
            pltpu.VMEM((local_count, LANES), jnp.float32),
            pltpu.VMEM((local_count * piece, LANES), jnp.float32),
            pltpu.VMEM((3 * orients, width), jnp.bfloat16),
            pltpu.VMEM((cands * orients, pair * width), jnp.bfloat16),
            pltpu.VMEM((2, half_rows, count), jnp.float32),
            pltpu.VMEM((2, half_rows, count // 2), jnp.float32),
            pltpu.VMEM((2, coded_rows, count // 2), jnp.int16),
            pltpu.VMEM((3, coded_rows, count // 4), jnp.int16),
            pltpu.VMEM((count // 4, columns), jnp.float32),
            pltpu.VMEM((count // 4, columns), jnp.int16),
            pltpu.VMEM((fars, local_count, columns), jnp.int16),
            pltpu.VMEM((local_count, columns), jnp.float32),
            pltpu.VMEM((local_count, columns), jnp.float32),
            pltpu.SemaphoreType.DMA((5,)),
            pltpu.SemaphoreType.DMA((3, tile_count)),
            pltpu.SemaphoreType.DMA((3, tile_count)),
            pltpu.SemaphoreType.DMA((4 + fars,)),
            pltpu.SemaphoreType.DMA((4 + fars,)),
            pltpu.SemaphoreType.DMA((2,)),
            pltpu.SemaphoreType.DMA((2,)),
        ],
        compiler_params=pltpu.CompilerParams(
            collective_id=0, has_side_effects=True, vmem_limit_bytes=56 * 1024 * 1024
        ),
        name="fused",
    )(
        view(particles),
        view(projections),
        noise_weight.reshape(-1, LANES),
        tile_list.T,
        ori_start.T,
        shifts.T,
        defocus_bin[None, :],
    )
    posterior, log_total = pl.pallas_call(
        settle_kernel,
        in_specs=[near_space] * 2,
        out_specs=[near_space] * 2,
        out_shape=[
            jax.ShapeDtypeStruct((cands, local_count, windows * (orients // 2)), jnp.float32),
            jax.ShapeDtypeStruct((1, local_count), jnp.float32),
        ],
        compiler_params=pltpu.CompilerParams(vmem_limit_bytes=4 * 1024 * 1024),
        name="settle",
    )(low, high)
    return jnp.transpose(posterior, (1, 0, 2)), log_total[0]


def fused_fits(particles, projections, tile_list):
    tile_count = lax.axis_size("tile")
    local_count, _, band_width = particles.shape
    return (
        lax.axis_size("shell") == 2
        and tile_count & (tile_count - 1) == 0
        and tile_count * local_count == 4 * LANES
        and band_width % (BOX * tile_count) == 0
        and projections.shape[0] == local_count
        and tile_list.shape[1] % 2 == 0
    )


def per_device(particles, projections, noise_weight, tile_list, ori_start, shifts, defocus_bin):
    plan = fused_plan if fused_fits(particles, projections, tile_list) else slot_plan
    return plan(
        particles, projections, noise_weight, tile_list, ori_start, shifts, defocus_bin
    )


def solution(mesh):
    in_specs = (
        P("tile", None, "shell"),
        P("tile", None, "shell"),
        P("shell"),
        P("tile", None),
        P("tile", None),
        P("tile", None),
        P("tile"),
    )
    out_specs = (P("tile", None, None), P("tile"))
    return jax.shard_map(
        per_device, mesh=mesh, in_specs=in_specs, out_specs=out_specs, check_vma=False
    )
```

```python
import functools
import math

import jax
import jax.numpy as jnp
from jax import lax
from jax.experimental import pallas as pl
from jax.experimental.pallas import tpu as pltpu
from jax.sharding import PartitionSpec as P

BOX = 256
NBIN = 16
TSIDE = 3


wave_length = 0.0197
aberration = 27000000.0
amplitude = 0.1
b_factor = 20.0
defocus_base = 5000.0
defocus_step = 500.0


def frequencies(first_index, span_count):
    flat_index = first_index + jnp.arange(span_count, dtype=jnp.int32)
    freq_x = flat_index // BOX
    freq_y = flat_index % BOX - BOX // 2
    return (freq_x, freq_y)


def ctf_table(freq_x, freq_y, bins_count):
    scaled_x = freq_x.astype(jnp.float32) / BOX
    scaled_y = freq_y.astype(jnp.float32) / BOX
    radius_sq = scaled_x * scaled_x + scaled_y * scaled_y
    defocus = defocus_base + defocus_step * jnp.arange(bins_count, dtype=jnp.float32)[:, None]
    aberr_phase = (
        math.pi * wave_length * defocus * radius_sq[None, :]
        - 0.5 * math.pi * aberration * wave_length**3 * radius_sq[None, :] ** 2
    )
    envelope = jnp.exp(-0.25 * b_factor * radius_sq)[None, :]
    return (
        -(math.sqrt(1.0 - amplitude**2) * jnp.sin(aberr_phase) + amplitude * jnp.cos(aberr_phase))
        * envelope
    )


def rotation(freq_x, freq_y, mult_x, mult_y):
    phase_turns = jnp.mod(freq_x * mult_x + freq_y * mult_y, BOX)
    angles = phase_turns.astype(jnp.float32) * (2.0 * math.pi / BOX)
    return (jnp.cos(angles), jnp.sin(angles))


def pick_rows(bin_index, lookup):
    one_hot = (bin_index[:, None] == jnp.arange(lookup.shape[0], dtype=jnp.int32)[None, :]).astype(
        jnp.float32
    )
    return jnp.dot(
        one_hot, lookup, precision=lax.Precision.HIGHEST, preferred_element_type=jnp.float32
    )


def prepare(particles, weight, ctf_rows, shifts, freq_x, freq_y):
    values = particles.astype(jnp.float32)
    real_part = values[:, 0]
    imag_part = values[:, 1]
    cosine, sine_value = rotation(freq_x[None, :], freq_y[None, :], shifts[:, 0:1], shifts[:, 1:2])
    moved_real = real_part * cosine + imag_part * sine_value
    moved_imag = imag_part * cosine - real_part * sine_value
    factor = weight[None, :] * ctf_rows
    weighted = jnp.stack([factor * moved_real, factor * moved_imag], axis=1).astype(jnp.bfloat16)
    energy = jnp.sum(weight[None, :] * (real_part * real_part + imag_part * imag_part), axis=1)
    return (weighted, energy)


def shifted_tables(projections, freq_x, freq_y):
    offsets = jnp.arange(TSIDE, dtype=jnp.int32) - TSIDE // 2
    mult_x = jnp.repeat(offsets, TSIDE)[:, None]
    mult_y = jnp.tile(offsets, TSIDE)[:, None]
    cosine, sine_value = rotation(freq_x[None, :], freq_y[None, :], mult_x, mult_y)
    cosine = cosine[:, None, :]
    sine_value = sine_value[:, None, :]
    proj_real = projections[:, 0].astype(jnp.float32)[None, :, :]
    proj_imag = projections[:, 1].astype(jnp.float32)[None, :, :]
    moved_real = proj_real * cosine - proj_imag * sine_value
    moved_imag = proj_imag * cosine + proj_real * sine_value
    stacked = jnp.stack([moved_real, moved_imag], axis=2).astype(jnp.bfloat16)
    return stacked.reshape(TSIDE * TSIDE * projections.shape[0], -1)


def slot_scores(slot_rows, bin_index, projections, weight, ctf, freq_x, freq_y):
    orient_count = projections.shape[0]
    lookup = shifted_tables(projections, freq_x, freq_y)
    cross_term = lax.dot_general(
        slot_rows, lookup, (((1,), (1,)), ((), ())), preferred_element_type=jnp.float32
    )
    cross_term = cross_term.reshape(slot_rows.shape[0], TSIDE * TSIDE, orient_count)
    proj_values = projections.astype(jnp.float32)
    magnitude = proj_values[:, 0] * proj_values[:, 0] + proj_values[:, 1] * proj_values[:, 1]
    weighted_ctf = weight[None, :] * ctf * ctf
    power = lax.dot_general(
        weighted_ctf,
        magnitude,
        (((1,), (1,)), ((), ())),
        precision=lax.Precision.HIGHEST,
        preferred_element_type=jnp.float32,
    )
    power_rows = pick_rows(bin_index, power)
    return cross_term - 0.5 * power_rows[:, None, :]


def window(scores, starts, orient_count):
    orient_index = jnp.mod(
        starts[:, None] + jnp.arange(orient_count // 2, dtype=jnp.int32)[None, :], orient_count
    )
    return jnp.take_along_axis(scores, orient_index[:, None, :], axis=2)


def slot_layout(tile_ids, tile_count, capacity):
    positions = jnp.arange(tile_ids.shape[0], dtype=jnp.int32)
    earlier_same = (tile_ids[:, None] == tile_ids[None, :]) & (
        positions[None, :] < positions[:, None]
    )
    slot_rank = jnp.sum(earlier_same.astype(jnp.int32), axis=1)
    slot_index = tile_ids * capacity + slot_rank
    matches = slot_index[None, :] == jnp.arange(tile_count * capacity, dtype=jnp.int32)[:, None]
    slot_owner = jnp.sum(jnp.where(matches, positions[None, :] + 1, 0), axis=1) - 1
    return (slot_index, slot_owner)


def finish(scores, energy_sum):
    scored = scores - 0.5 * energy_sum[:, None, None]
    row_peak = jnp.max(scored, axis=(1, 2))
    log_total = row_peak + jnp.log(jnp.sum(jnp.exp(scored - row_peak[:, None, None]), axis=(1, 2)))
    posterior = jnp.exp(scored - log_total[:, None, None])
    return (posterior, log_total)


def slot_plan(particles, projections, noise_weight, tile_list, ori_start, shifts, defocus_bin):
    tile_count = lax.axis_size("tile")
    band_index = lax.axis_index("shell")
    local_count = particles.shape[0]
    window_count = tile_list.shape[1]
    band_width = particles.shape[2]
    orient_count = projections.shape[0]
    capacity = max(2, (2 * local_count * window_count + tile_count - 1) // tile_count)
    freq_x, freq_y = frequencies(band_index * band_width, band_width)
    ctf = ctf_table(freq_x, freq_y, NBIN)
    weighted, energy = prepare(
        particles, noise_weight, pick_rows(defocus_bin, ctf), shifts, freq_x, freq_y
    )
    weighted = weighted.reshape(local_count, 2 * band_width)
    slot_index, slot_owner = slot_layout(tile_list.reshape(-1), tile_count, capacity)
    occupied = slot_owner >= 0
    item_index = jnp.maximum(slot_owner, 0)
    particle = item_index // window_count
    starts_flat = ori_start.reshape(-1)
    send_rows = jnp.where(
        occupied[:, None], jnp.take(weighted, particle, axis=0), jnp.zeros((), jnp.bfloat16)
    )
    send_rows = send_rows.reshape(tile_count, capacity, 2 * band_width)
    send_labels = jnp.stack(
        [jnp.take(defocus_bin, particle), jnp.take(starts_flat, item_index)], axis=1
    )
    send_labels = send_labels.astype(jnp.bfloat16).reshape(tile_count, capacity, 2)
    payload = lax.all_to_all(send_rows, "tile", split_axis=0, concat_axis=0, tiled=True)
    labels = lax.all_to_all(send_labels, "tile", split_axis=0, concat_axis=0, tiled=True)
    source_count = payload.shape[0]
    slot_count = payload.shape[1]
    slot_rows = payload.reshape(source_count * slot_count, payload.shape[2])
    label_ints = labels.reshape(source_count * slot_count, 2).astype(jnp.int32)
    partial_value = slot_scores(
        slot_rows, label_ints[:, 0], projections, noise_weight, ctf, freq_x, freq_y
    )
    partial_value = partial_value.reshape(
        source_count, slot_count, partial_value.shape[1], partial_value.shape[2]
    )
    returned = lax.all_to_all(partial_value, "tile", split_axis=0, concat_axis=0, tiled=True)
    candidates = returned.shape[2]
    returned = jnp.take(
        returned.reshape(tile_count * capacity, candidates, returned.shape[3]), slot_index, axis=0
    )
    returned = window(returned, starts_flat, orient_count)
    kept = returned.shape[2]
    returned = returned.reshape(local_count, window_count, candidates, kept)
    scores = jnp.transpose(returned, (0, 2, 1, 3)).reshape(
        local_count, candidates, window_count * kept
    )
    scores, energy_sum = lax.psum((scores, energy), "shell")
    return finish(scores, energy_sum)


SHIFT_MAX = 8
HIGH = lax.Precision.HIGHEST


def round_up(value, step):
    return (value + step - 1) // step * step


LANES = 128
CODE_TOP = 32000.0
MESH = pl.DeviceIdType.MESH


def flip(index, turn, count):
    result = index
    step = 1
    while step < count:
        result = result + step * (turn // step % 2) * (1 - 2 * (index // step % 2))
        step *= 2
    return result


def slot_of(order, fars):
    late = (order // 4 + fars - 1) // fars
    rest = late * (order - 4)
    far = late * (fars - 1 - rest % (fars - 1))
    near = late * (rest // (fars - 1)) + (1 - late) * order
    return far, near


def offset_of(order, fars):
    far, near = slot_of(order, fars)
    return far * 4 + near


def place_of(order, fars):
    far, near = slot_of(order, fars)
    return (near % 2 * 2 + near // 2) * fars + far


def turn_pair(phase):
    angle = (phase & (BOX - 1)).astype(jnp.float32) * (2.0 * math.pi / BOX)
    return jnp.cos(angle), jnp.sin(angle)


def three(value):
    parts = []
    for _ in range(3):
        part = value.astype(jnp.bfloat16)
        value = value - part.astype(jnp.float32)
        parts.append(part)
    return parts


def fused_kernel(
    part_ref,
    proj_ref,
    noise_ref,
    tiles_ref,
    starts_ref,
    shifts_ref,
    bins_ref,
    low_ref,
    high_ref,
    label_row,
    label_ref,
    weight_ref,
    turn_y_ref,
    turn_x_ref,
    ctf_ref,
    power_ref,
    cos_ref,
    sin_ref,
    part_in,
    proj_in,
    label_in,
    hot_parts,
    wave_y,
    wave_x,
    factor,
    weighted,
    local_part,
    local_noise,
    noise_rows,
    square_sum,
    plain,
    magnitude,
    moved,
    sums,
    core_in,
    side_out,
    side_in,
    far_sum,
    far_out,
    far_in,
    pair_out,
    pair_in,
    own_sems,
    send_sems,
    recv_sems,
    back_send,
    back_recv,
    core_send,
    core_recv,
):
    tile_count, rows, lines, _ = part_in.shape
    fars = tile_count // 4
    orients = proj_in.shape[1]
    kept = orients // 2
    cands = TSIDE * TSIDE
    middle = cands // 2
    windows = tiles_ref.shape[0]
    chunks = weight_ref.shape[0]
    width = chunks * LANES
    band_rows = width // BOX
    count = weighted.shape[0]
    half_windows = windows // 2
    used = cands * half_windows * kept
    me = lax.axis_index("tile")
    band = lax.axis_index("shell")
    other = 1 - band
    core_peer = flip(me, 1, tile_count)
    side_peer = flip(me, 2, tile_count)

    barrier = pltpu.get_barrier_semaphore()
    peers = [(flip(me, offset, tile_count), band) for offset in range(1, tile_count)]
    peers += [(me, other), (side_peer, other)]
    for peer in peers:
        pl.semaphore_signal(barrier, inc=1, device_id=peer, device_id_type=MESH)
    label_row[...] = jnp.zeros_like(label_row)
    first = 0
    for ref in (tiles_ref, starts_ref, shifts_ref, bins_ref):
        label_row[first : first + ref.shape[0], :rows] = ref[...].astype(jnp.float32)
        first += ref.shape[0]
    for far in range(fars):
        moved_row = pltpu.roll(label_row[...], far * rows, 1) if far else label_row[...]
        label_ref[far] = moved_row.astype(jnp.bfloat16)
    pl.semaphore_wait(barrier, len(peers))

    def remote(source, target, send, recv, peer):
        return pltpu.make_async_remote_copy(
            src_ref=source,
            dst_ref=target,
            send_sem=send,
            recv_sem=recv,
            device_id=peer,
            device_id_type=MESH,
        )

    def piece(ref, tile):
        return ref.at[:, pl.ds(pl.multiple_of(tile * lines, lines), lines), :]

    sent = []
    own_copies = []
    for kind, (source, target) in enumerate(
        ((label_ref, label_in), (part_ref, part_in), (proj_ref, proj_in))
    ):
        if kind:
            copy = pltpu.make_async_copy(piece(source, me), target.at[0], own_sems.at[kind - 1])
            copy.start()
            own_copies.append(copy)
        for order in range(1, tile_count):
            tile = flip(me, offset_of(order, fars), tile_count)
            block = piece(source, tile) if kind else source.at[place_of(order, fars) % fars]
            copy = remote(
                block,
                target.at[order],
                send_sems.at[kind, order],
                recv_sems.at[kind, order],
                (tile, band),
            )
            copy.start()
            sent.append(copy)

    def arrived(kind, target, order):
        remote(
            target.at[order],
            target.at[order],
            send_sems.at[kind, order],
            recv_sems.at[kind, order],
            (core_peer, band),
        ).wait_recv()

    noise = pltpu.make_async_copy(
        noise_ref.at[pl.ds(pl.multiple_of(me * chunks, chunks), chunks), :],
        weight_ref,
        own_sems.at[2],
    )
    noise.start()
    own_copies.append(noise)
    local_copies = [
        pltpu.make_async_copy(part_ref, local_part, own_sems.at[3]),
        pltpu.make_async_copy(noise_ref, local_noise, own_sems.at[4]),
    ]
    for copy in local_copies:
        copy.start()

    sums[...] = jnp.zeros_like(sums)
    first_line = (band * tile_count + me) * band_rows
    steps = turn_y_ref.shape[0]
    shape = (steps, BOX)
    step = lax.broadcasted_iota(jnp.int32, shape, 0) - SHIFT_MAX
    freq = lax.broadcasted_iota(jnp.int32, shape, 1) - BOX // 2
    cosine, sine_value = turn_pair(step * freq)
    turn_y_ref[:, :BOX] = cosine
    turn_y_ref[:, BOX:] = sine_value
    shape = (steps, LANES)
    step = lax.broadcasted_iota(jnp.int32, shape, 0) - SHIFT_MAX
    line = lax.broadcasted_iota(jnp.int32, shape, 1)
    swap = line >= band_rows
    cosine, sine_value = turn_pair(step * (first_line + jnp.where(swap, line - band_rows, line)))
    turn_x_ref[...] = jnp.where(swap, sine_value, cosine)
    shape = (cos_ref.shape[0], width)
    cand = lax.broadcasted_iota(jnp.int32, shape, 0)
    flat = lax.broadcasted_iota(jnp.int32, shape, 1)
    mult_x = jnp.zeros(shape, jnp.int32)
    for turn in range(1, TSIDE):
        mult_x = mult_x + (cand >= turn * TSIDE).astype(jnp.int32)
    mult_y = cand - TSIDE * mult_x - TSIDE // 2
    mult_x = mult_x - TSIDE // 2
    freq_x = first_line + (flat >> (BOX.bit_length() - 1))
    freq_y = (flat & (BOX - 1)) - BOX // 2
    cosine, sine_value = turn_pair(freq_x * mult_x + freq_y * mult_y)
    cos_ref[...] = cosine
    sin_ref[...] = sine_value
    for copy in own_copies:
        copy.wait()
    shape = (NBIN, LANES)
    defocus_bin = lax.broadcasted_iota(jnp.int32, shape, 0).astype(jnp.float32)
    defocus = defocus_base + defocus_step * defocus_bin
    for chunk in range(chunks):
        line, side = divmod(chunk, BOX // LANES)
        lane = lax.broadcasted_iota(jnp.int32, shape, 1) + (side * LANES - BOX // 2)
        scaled_x = (first_line + line).astype(jnp.float32) / BOX
        scaled_y = lane.astype(jnp.float32) / BOX
        radius_sq = scaled_x * scaled_x + scaled_y * scaled_y
        aberr_phase = (
            math.pi * wave_length * defocus * radius_sq
            - 0.5 * math.pi * aberration * wave_length**3 * radius_sq**2
        )
        envelope = jnp.exp(-0.25 * b_factor * radius_sq)
        ctf = -(
            math.sqrt(1.0 - amplitude**2) * jnp.sin(aberr_phase) + amplitude * jnp.cos(aberr_phase)
        )
        ctf = ctf * envelope
        columns = slice(chunk * LANES, (chunk + 1) * LANES)
        ctf_ref[:, columns] = weight_ref[chunk : chunk + 1, :] * ctf
        for part, value in enumerate(three(0.5 * weight_ref[chunk : chunk + 1, :] * ctf * ctf)):
            power_ref[part * NBIN : (part + 1) * NBIN, columns] = value

    label_in[0] = label_ref[0]
    for order in range(1, tile_count):
        arrived(0, label_in, order)
    groups = [jnp.zeros(label_in.shape[1:], jnp.float32)] * 4
    for order in range(tile_count):
        group = place_of(order, fars) // fars
        groups[group] = groups[group] + label_in[order].astype(jnp.float32)
    labels = jnp.concatenate(groups, axis=1)
    tiles = [labels[j : j + 1] for j in range(windows)]
    starts = [labels[windows + j : windows + j + 1] for j in range(windows)]
    shift_x = labels[2 * windows : 2 * windows + 1]
    shift_y = labels[2 * windows + 1 : 2 * windows + 2]
    bins = labels[2 * windows + 2 : 2 * windows + 3]

    def one_hot(row, table_rows, base):
        index = lax.broadcasted_iota(jnp.int32, (table_rows, count), 0).astype(jnp.float32)
        return (index == row + base).astype(jnp.float32)

    def pick(one_hots, table):
        return lax.dot_general(
            one_hots,
            table,
            (((0,), (0,)), ((), ())),
            precision=HIGH,
            preferred_element_type=jnp.float32,
        )

    hot = one_hot(bins, NBIN, 0.0)
    hot_parts[...] = jnp.concatenate([hot] * 3, axis=0).astype(jnp.bfloat16)
    wave_y[...] = pick(one_hot(shift_y, steps, float(SHIFT_MAX)), turn_y_ref[...])
    wave_x[...] = pick(one_hot(shift_x, steps, float(SHIFT_MAX)), turn_x_ref[...])
    factor[...] = pick(hot, ctf_ref[...])

    for copy in local_copies:
        copy.wait()
    pairs = local_noise.shape[0]
    for part in range(2):
        noise_rows[pl.ds(part, pairs, stride=2), :] = local_noise[...]

    def square(particle, carry):
        total = jnp.zeros((8, LANES), jnp.float32)
        for first in range(0, 2 * pairs, 16):
            value = local_part[particle, first : first + 16, :].astype(jnp.float32)
            value = value * value * noise_rows[first : first + 16, :]
            total = total + value[:8] + value[8:]
        square_sum[pl.ds(particle, 1), :] = jnp.sum(total, axis=0, keepdims=True)
        return carry

    lax.fori_loop(0, rows, square, 0)

    def unpack(value):
        plain[...] = value.reshape(rows * lines, LANES).astype(jnp.float32)

    def parts_of(chunk):
        real_part = plain[pl.ds(2 * chunk, rows, stride=lines), :]
        imag_part = plain[pl.ds(2 * chunk + 1, rows, stride=lines), :]
        return real_part, imag_part

    def weigh(order, carry):
        @pl.when(order > 0)
        def _():
            arrived(1, part_in, order)

        unpack(part_in[order])
        first = pl.multiple_of(place_of(order, fars) * rows, rows)
        span = pl.ds(first, rows)
        for chunk in range(chunks):
            line, side = divmod(chunk, BOX // LANES)
            real_part, imag_part = parts_of(chunk)
            cos_y = wave_y[span, side * LANES : (side + 1) * LANES]
            sin_y = wave_y[span, BOX + side * LANES : BOX + (side + 1) * LANES]
            cos_x = wave_x[span, line : line + 1]
            sin_x = wave_x[span, band_rows + line : band_rows + line + 1]
            cosine = cos_x * cos_y - sin_x * sin_y
            sine_value = sin_x * cos_y + cos_x * sin_y
            columns = slice(chunk * LANES, (chunk + 1) * LANES)
            scale = factor[span, columns]
            weighted[span, columns] = (
                scale * (real_part * cosine + imag_part * sine_value)
            ).astype(jnp.bfloat16)
            weighted[span, width + chunk * LANES : width + (chunk + 1) * LANES] = (
                scale * (imag_part * cosine - real_part * sine_value)
            ).astype(jnp.bfloat16)
        return carry

    lax.fori_loop(0, tile_count, weigh, 0)

    def score(order, carry):
        @pl.when(order > 0)
        def _():
            arrived(2, proj_in, order)

        unpack(proj_in[order])
        for chunk in range(chunks):
            columns = slice(chunk * LANES, (chunk + 1) * LANES)
            real_part, imag_part = parts_of(chunk)
            for part, value in enumerate(three(real_part * real_part + imag_part * imag_part)):
                magnitude[part * orients : (part + 1) * orients, columns] = value

            def put(cand, real_value, imag_value):
                span = slice(cand * orients, (cand + 1) * orients)
                moved[span, columns] = real_value.astype(jnp.bfloat16)
                moved[span, width + chunk * LANES : width + (chunk + 1) * LANES] = (
                    imag_value.astype(jnp.bfloat16)
                )

            put(middle, real_part, imag_part)
            for cand in range(middle):
                cosine = cos_ref[cand : cand + 1, columns]
                sine_value = sin_ref[cand : cand + 1, columns]
                real_cos = real_part * cosine
                imag_sin = imag_part * sine_value
                imag_cos = imag_part * cosine
                real_sin = real_part * sine_value
                put(cand, real_cos - imag_sin, imag_cos + real_sin)
                put(cands - 1 - cand, real_cos + imag_sin, imag_cos - real_sin)
        power = lax.dot_general(
            magnitude[...],
            power_ref[...],
            (((1,), (1,)), ((), ())),
            preferred_element_type=jnp.float32,
        )
        power = power[:orients] + power[orients : 2 * orients] + power[2 * orients :]
        half_power = jnp.dot(
            jnp.concatenate(three(power), axis=0),
            hot_parts[...],
            preferred_element_type=jnp.float32,
        )
        half_power = (
            half_power[:orients] + half_power[orients : 2 * orients] + half_power[2 * orients :]
        )
        cross = lax.dot_general(
            moved[...],
            weighted[...],
            (((1,), (1,)), ((), ())),
            preferred_element_type=jnp.float32,
        )
        tile = flip(me, offset_of(order, fars), tile_count).astype(jnp.float32)
        named = [row == tile for row in tiles]
        start = jnp.zeros_like(starts[0])
        for j in range(windows):
            start = jnp.where(named[j], starts[j], start)
        start = start.astype(jnp.int32)
        for cand in range(cands):
            value = cross[cand * orients : (cand + 1) * orients] - half_power
            bit = orients // 2
            while bit:
                turned = pltpu.roll(value, orients - bit, 0)
                value = jnp.where((start & bit) != 0, turned, value)
                bit //= 2
            value = value[:kept]
            for j in range(windows):
                half, place = divmod(j, half_windows)
                first = (cand * half_windows + place) * kept
                span = slice(first, first + kept)
                sums[half, span, :] = jnp.where(named[j], value, sums[half, span, :])
        return carry

    lax.fori_loop(0, tile_count, score, 0)

    near = count // 2
    quarter = count // 4
    core_copies = []
    for turn, half in enumerate((other, band)):
        copy = remote(
            sums.at[half, :, pl.ds(near, near)],
            core_in.at[half],
            core_send.at[turn],
            core_recv.at[turn],
            (core_peer, band),
        )
        copy.start()
        core_copies.append(copy)
    sent += core_copies

    def scale_of(peak):
        return jnp.ceil(jnp.log2(jnp.maximum(peak, 1e-30)))

    def coded(value, scale):
        return jnp.round(value * (CODE_TOP * jnp.exp2(-scale))).astype(jnp.int32)

    def plain_of(code, scale):
        return code.astype(jnp.float32) * (jnp.exp2(scale) / CODE_TOP)

    scale_rows = side_out.shape[1] - used
    copies = []
    for turn, half in enumerate((other, band)):
        core_copies[turn].wait_recv()
        whole = sums[half, :, :near] + core_in[half]
        sums[half, :, :near] = whole
        scale = scale_of(jnp.max(jnp.abs(whole), axis=0, keepdims=True))
        side_out[half, :used, :] = coded(whole, scale).astype(jnp.int16)
        side_out[half, used:, :] = (
            jnp.broadcast_to(scale, (scale_rows, near)).astype(jnp.int32).astype(jnp.int16)
        )
        ways = ((1, (side_peer, other)), (0, (me, other))) if turn == 0 else ((1, (side_peer, band)),)
        for lane, peer in ways:
            way = len(copies)
            copy = remote(
                side_out.at[half, :, pl.ds(lane * quarter, quarter)],
                side_in.at[way],
                back_send.at[1 + way],
                back_recv.at[1 + way],
                peer,
            )
            copy.start()
            copies.append(copy)
    total = sums[band, :, :quarter]
    for way, copy in enumerate(copies):
        copy.wait_recv()
        code = side_in[way].astype(jnp.int32)
        total = total + plain_of(code[:used], code[used : used + 1].astype(jnp.float32))
    sent += copies
    columns = far_out.shape[1]
    total = jnp.concatenate([total, jnp.zeros((columns - used, quarter), jnp.float32)], axis=0)
    total = total.T
    far_sum[...] = total
    scale = scale_of(jnp.max(jnp.abs(total), axis=1, keepdims=True))
    column = lax.broadcasted_iota(jnp.int32, total.shape, 1)
    code = coded(total, scale)
    far_out[...] = jnp.where(column >= used, scale.astype(jnp.int32), code).astype(jnp.int16)

    copies = []
    for far in range(fars - 1, 0, -1):
        copy = remote(
            far_out.at[pl.ds(far * rows, rows), :],
            far_in.at[far],
            back_send.at[3 + far],
            back_recv.at[3 + far],
            (flip(me, 4 * far, tile_count), band),
        )
        copy.start()
        copies.append(copy)
    energy = jnp.sum(square_sum[...], axis=1, keepdims=True)
    total = far_sum[:rows, :]
    for far, copy in enumerate(copies):
        copy.wait_recv()
        code = far_in[fars - 1 - far].astype(jnp.int32)
        total = total + plain_of(code, code[:, used : used + 1].astype(jnp.float32))
    sent += copies
    column = lax.broadcasted_iota(jnp.int32, total.shape, 1)
    total = jnp.where(column >= used, energy, total)
    pair_out[...] = total
    copy = remote(
        pair_out, pair_in, back_send.at[3 + fars], back_recv.at[3 + fars], (me, other)
    )
    copy.start()
    sent.append(copy)
    copy.wait_recv()
    theirs = pair_in[...]
    low_ref[...] = jnp.where(band == 0, total, theirs)
    high_ref[...] = jnp.where(band == 0, theirs, total)
    for copy in sent:
        copy.wait_send()


def settle_kernel(low_ref, high_ref, post_ref, log_ref):
    cands, rows, span = post_ref.shape
    used = cands * span // 2
    low = low_ref[...]
    high = high_ref[...]
    inside = lax.broadcasted_iota(jnp.int32, low.shape, 1) < used
    least = jnp.full_like(low, -jnp.inf)
    energy = low[:, used : used + 1] + high[:, used : used + 1]
    low = jnp.where(inside, low, least)
    high = jnp.where(inside, high, least)
    peak = jnp.max(jnp.maximum(low, high), axis=1, keepdims=True)
    mass = jnp.sum(jnp.exp(low - peak) + jnp.exp(high - peak), axis=1, keepdims=True)
    log_total = peak + jnp.log(mass)
    low = jnp.exp(low - log_total)
    high = jnp.exp(high - log_total)
    half = span // 2
    for cand in range(cands):
        columns = slice(cand * half, (cand + 1) * half)
        post_ref[cand] = jnp.concatenate([low[:, columns], high[:, columns]], axis=1)
    evidence = jnp.broadcast_to(log_total - 0.5 * energy, (rows, LANES))
    log_ref[...] = evidence.T[:1, :]


def fused_plan(particles, projections, noise_weight, tile_list, ori_start, shifts, defocus_bin):
    tile_count = lax.axis_size("tile")
    local_count, pair, band_width = particles.shape
    orients = projections.shape[0]
    windows = tile_list.shape[1]
    width = band_width // tile_count
    count = local_count * tile_count
    cands = TSIDE * TSIDE
    fars = tile_count // 4
    half_rows = cands * (windows // 2) * (orients // 2)
    coded_rows = half_rows + 16
    columns = round_up(half_rows + 1, LANES)
    piece = width // LANES * pair

    label_rows = round_up(2 * windows + shifts.shape[1] + 1, 16)
    steps = round_up(2 * SHIFT_MAX + 1, 8)
    half_cands = round_up(cands // 2, 8)

    def view(values):
        rows = values.shape[0]
        blocks = values.reshape(rows, pair, band_width // LANES, LANES)
        return jnp.transpose(blocks, (0, 2, 1, 3)).reshape(rows, -1, LANES)

    far_space = pl.BlockSpec(memory_space=pl.ANY)
    near_space = pl.BlockSpec(memory_space=pltpu.VMEM)
    low, high = pl.pallas_call(
        fused_kernel,
        in_specs=[far_space] * 3 + [near_space] * 4,
        out_specs=[near_space] * 2,
        out_shape=[pltpu.VMEM((local_count, columns), jnp.float32)] * 2,
        scratch_shapes=[
            pltpu.VMEM((label_rows, LANES), jnp.float32),
            pltpu.VMEM((fars, label_rows, LANES), jnp.bfloat16),
            pltpu.VMEM((width // LANES, LANES), jnp.float32),
            pltpu.VMEM((steps, 2 * BOX), jnp.float32),
            pltpu.VMEM((steps, LANES), jnp.float32),
            pltpu.VMEM((NBIN, width), jnp.float32),
            pltpu.VMEM((3 * NBIN, width), jnp.bfloat16),
            pltpu.VMEM((half_cands, width), jnp.float32),
            pltpu.VMEM((half_cands, width), jnp.float32),
            pltpu.VMEM((tile_count, local_count, piece, LANES), jnp.bfloat16),
            pltpu.VMEM((tile_count, orients, piece, LANES), jnp.bfloat16),
            pltpu.VMEM((tile_count, label_rows, LANES), jnp.bfloat16),
            pltpu.VMEM((3 * NBIN, count), jnp.bfloat16),
            pltpu.VMEM((count, 2 * BOX), jnp.float32),
            pltpu.VMEM((count, LANES), jnp.float32),
            pltpu.VMEM((count, width), jnp.float32),
            pltpu.VMEM((count, pair * width), jnp.bfloat16),
            pltpu.VMEM((local_count, band_width // LANES * pair, LANES), jnp.bfloat16),
            pltpu.VMEM((band_width // LANES, LANES), jnp.float32),
            pltpu.VMEM((band_width // LANES * pair, LANES), jnp.float32),
            pltpu.VMEM((local_count, LANES), jnp.float32),
            pltpu.VMEM((local_count * piece, LANES), jnp.float32),
            pltpu.VMEM((3 * orients, width), jnp.bfloat16),
            pltpu.VMEM((cands * orients, pair * width), jnp.bfloat16),
            pltpu.VMEM((2, half_rows, count), jnp.float32),
            pltpu.VMEM((2, half_rows, count // 2), jnp.float32),
            pltpu.VMEM((2, coded_rows, count // 2), jnp.int16),
            pltpu.VMEM((3, coded_rows, count // 4), jnp.int16),
            pltpu.VMEM((count // 4, columns), jnp.float32),
            pltpu.VMEM((count // 4, columns), jnp.int16),
            pltpu.VMEM((fars, local_count, columns), jnp.int16),
            pltpu.VMEM((local_count, columns), jnp.float32),
            pltpu.VMEM((local_count, columns), jnp.float32),
            pltpu.SemaphoreType.DMA((5,)),
            pltpu.SemaphoreType.DMA((3, tile_count)),
            pltpu.SemaphoreType.DMA((3, tile_count)),
            pltpu.SemaphoreType.DMA((4 + fars,)),
            pltpu.SemaphoreType.DMA((4 + fars,)),
            pltpu.SemaphoreType.DMA((2,)),
            pltpu.SemaphoreType.DMA((2,)),
        ],
        compiler_params=pltpu.CompilerParams(
            collective_id=0, has_side_effects=True, vmem_limit_bytes=56 * 1024 * 1024
        ),
        name="fused",
    )(
        view(particles),
        view(projections),
        noise_weight.reshape(-1, LANES),
        tile_list.T,
        ori_start.T,
        shifts.T,
        defocus_bin[None, :],
    )
    posterior, log_total = pl.pallas_call(
        settle_kernel,
        in_specs=[near_space] * 2,
        out_specs=[near_space] * 2,
        out_shape=[
            jax.ShapeDtypeStruct((cands, local_count, windows * (orients // 2)), jnp.float32),
            jax.ShapeDtypeStruct((1, local_count), jnp.float32),
        ],
        compiler_params=pltpu.CompilerParams(vmem_limit_bytes=4 * 1024 * 1024),
        name="settle",
    )(low, high)
    return jnp.transpose(posterior, (1, 0, 2)), log_total[0]


def fused_fits(particles, projections, tile_list):
    tile_count = lax.axis_size("tile")
    local_count, _, band_width = particles.shape
    return (
        lax.axis_size("shell") == 2
        and tile_count & (tile_count - 1) == 0
        and tile_count * local_count == 4 * LANES
        and band_width % (BOX * tile_count) == 0
        and projections.shape[0] == local_count
        and tile_list.shape[1] % 2 == 0
    )


def per_device(particles, projections, noise_weight, tile_list, ori_start, shifts, defocus_bin):
    plan = fused_plan if fused_fits(particles, projections, tile_list) else slot_plan
    return plan(
        particles, projections, noise_weight, tile_list, ori_start, shifts, defocus_bin
    )


def solution(mesh):
    in_specs = (
        P("tile", None, "shell"),
        P("tile", None, "shell"),
        P("shell"),
        P("tile", None),
        P("tile", None),
        P("tile", None),
        P("tile"),
    )
    out_specs = (P("tile", None, None), P("tile"))
    return jax.shard_map(
        per_device, mesh=mesh, in_specs=in_specs, out_specs=out_specs, check_vma=False
    )
```
